32 devices in a mesh: fsdp: 4 (over z), ctx: 4 (over y, x), tp: 2 (over core).
Axes of the slice: x: 2, y: 2, z: 4, core: 2. Of those that a mesh axis runs over, the one named last changes fastest.
Arguments:
- layer_input: bfloat16 [2048, 8, 768], P('ctx', 'fsdp'), may hold values from -6 to 6
- output_cotangent: bfloat16 [2048, 8, 768], P('ctx', 'fsdp'), may hold values from -6 to 6
- prefix_len: int32 [8], P('fsdp'), may hold values from 204 to 1024, as said below
- attn_gain: float32 [768], P('fsdp'), may hold values from 0.25 to 1.75
- mlp_gain: float32 [768], P('fsdp'), may hold values from 0.25 to 1.75
- query_weight: float32 [768, 768], P('fsdp', 'tp'), may hold values from -0.21875 to 0.21875
- key_weight: float32 [768, 768], P('fsdp', 'tp'), may hold values from -0.21875 to 0.21875
- value_weight: float32 [768, 768], P('fsdp', 'tp'), may hold values from -0.21875 to 0.21875
- out_weight: float32 [768, 768], P('tp', 'fsdp'), may hold values from -4.8 to 4.8
- gate_weight: float32 [768, 2048], P('fsdp', 'tp'), may hold values from -0.21875 to 0.21875
- up_weight: float32 [768, 2048], P('fsdp', 'tp'), may hold values from -0.21875 to 0.21875
- down_weight: float32 [2048, 768], P('tp', 'fsdp'), may hold values from -0.125 to 0.125
Outputs:
- layer_output: bfloat16 [2048, 8, 768], P('ctx', 'fsdp')
- input_grad: bfloat16 [2048, 8, 768], P('ctx', 'fsdp')
- attn_gain_grad: float32 [768], P('fsdp')
- mlp_gain_grad: float32 [768], P('fsdp')
- query_weight_grad: float32 [768, 768], P('fsdp', 'tp')
- key_weight_grad: float32 [768, 768], P('fsdp', 'tp')
- value_weight_grad: float32 [768, 768], P('fsdp', 'tp')
- out_weight_grad: float32 [768, 768], P('tp', 'fsdp')
- gate_weight_grad: float32 [768, 2048], P('fsdp', 'tp')
- up_weight_grad: float32 [768, 2048], P('fsdp', 'tp')
- down_weight_grad: float32 [2048, 768], P('tp', 'fsdp')
The draws below stay inside these ranges and needn't reach their ends.
Inputs may be any that keep to these rules, and one draw needn't show every extreme that they name: `prefix_len`: number of leading positions of each sequence that all its queries see; one sequence has each bound.
All inputs are finite; a program needn't handle non-finite values.
Results may differ from the reference program's by a relative error of at most 0.025.
Values may be sent and summed in bfloat16 or wider, within the bound.
A program may use at most 128 MiB of HBM per device.

```python
import math
import jax
import jax.numpy as jnp
from jax import lax

D = 768
HEADS = 12
HEAD_DIM = 64
FF = 2048
SEQS = 8
LEN = 2048


def draw_prefix_len(key, part):
    lowest = LEN // 10
    highest = LEN // 2
    key_values, key_order = jax.random.split(key)
    lengths = jax.random.randint(key_values, (SEQS,), lowest, highest + 1, dtype=jnp.int32)
    shuffled = jax.random.permutation(key_order, SEQS)
    lengths = lengths.at[shuffled[0]].set(highest)
    lengths = lengths.at[shuffled[1]].set(lowest)
    return lengths


def block_scale(own_key, dims, shards, least, high):
    loudness, own = 1.0, jax.random.fold_in(own_key, 6)
    for axis_at, parts in shards:
        steps = jnp.exp(jax.random.uniform(jax.random.fold_in(own, axis_at), (parts,), jnp.float32, least / len(shards), high / len(shards)))
        loudness = loudness * jnp.repeat(steps, dims[axis_at] // parts).reshape([-1 if axis == axis_at else 1 for axis in range(len(dims))])
    return loudness


def centred(rng, shape, scale, limit, shards=(), kind=jnp.bfloat16):
    drawn = jax.random.normal(rng, shape, jnp.float32) * scale
    if len(shards) > 0:
        drawn = block_scale(rng, shape, shards, -0.22, 0.18) * drawn
    return jnp.clip(drawn, min=-limit, max=limit).astype(kind)


def setup_inputs(seed: int = 0) -> dict:
    splits = jax.random.split(jax.random.key(seed), 13)
    return {
        "layer_input": centred(splits[0], (LEN, SEQS, D), 1.0, 6.0, ((0, 4), (1, 4))),
        "output_cotangent": centred(splits[1], (LEN, SEQS, D), 1.0, 6.0, ((0, 4), (1, 4))),
        "prefix_len": draw_prefix_len(jax.random.fold_in(splits[12], 71), 0),
        "attn_gain": jnp.clip(1.0 + 0.15 * jax.random.normal(splits[3], (D,), jnp.float32), 0.25, 1.75),
        "mlp_gain": jnp.clip(1.0 + 0.15 * jax.random.normal(splits[4], (D,), jnp.float32), 0.25, 1.75),
        "query_weight": centred(splits[5], (D, D), D ** -0.5, 0.21875, ((0, 4), (1, 2)), jnp.float32),
        "key_weight": centred(splits[6], (D, D), D ** -0.5, 0.21875, ((0, 4), (1, 2)), jnp.float32),
        "value_weight": centred(splits[7], (D, D), D ** -0.5, 0.21875, ((0, 4), (1, 2)), jnp.float32),
        "out_weight": centred(splits[8], (D, D), 0.8, 4.8, ((0, 2), (1, 4)), jnp.float32),
        "gate_weight": centred(splits[9], (D, FF), D ** -0.5, 0.21875, ((0, 4), (1, 2)), jnp.float32),
        "up_weight": centred(splits[10], (D, FF), D ** -0.5, 0.21875, ((0, 4), (1, 2)), jnp.float32),
        "down_weight": centred(splits[11], (FF, D), FF ** -0.5, 0.125, ((0, 2), (1, 4)), jnp.float32),
    }


EPS = 1e-06
BASE = 10000.0
MASKED = -1e+30

@jax.custom_vjp
def low(v):
    return lax.optimization_barrier(v.astype(jnp.bfloat16)).astype(jnp.float32)

@jax.custom_vjp
def low_back(v):
    return v

def low_keep(v):
    return (low(v), None)

def low_pass(kept, grad):
    return (grad,)

def back_keep(v):
    return (v, None)

def back_low(kept, grad):
    return (low(grad),)
low.defvjp(low_keep, low_pass)
low_back.defvjp(back_keep, back_low)

def matmul_high(left, right):
    return jnp.dot(left, right, precision=lax.Precision.HIGHEST, preferred_element_type=jnp.float32)

def norm_rows(values, gain):
    return values * lax.rsqrt(lax.optimization_barrier(jnp.mean(values * values, axis=-1, keepdims=True)) + EPS) * gain

def rope_tables(length):
    half_dim = HEAD_DIM // 2
    frequency = jnp.exp(jnp.arange(half_dim, dtype=jnp.float32) * (-2.0 * math.log(BASE) / HEAD_DIM))
    angles = jnp.arange(length, dtype=jnp.float32)[:, None] * frequency[None, :]
    cos_table = jnp.concatenate([jnp.cos(angles), jnp.cos(angles)], axis=1)
    sine_table = jnp.concatenate([jnp.sin(angles), jnp.sin(angles)], axis=1)
    return (cos_table, sine_table)

def rotate(values):
    half_dim = values.shape[-1] // 2
    return jnp.concatenate([-values[..., half_dim:], values[..., :half_dim]], axis=-1)

def attention(queries, key_heads, value_heads, prefix):
    length = queries.shape[0]
    block_rows = min(512, length)
    key_pos = jnp.arange(length, dtype=jnp.int32)
    query_blocks = queries.reshape(length // block_rows, block_rows, HEADS, HEAD_DIM)
    block_starts = jnp.arange(length // block_rows, dtype=jnp.int32) * block_rows

    @jax.checkpoint
    def one_block(element):
        query_block, block_start = element
        query_pos = block_start + jnp.arange(block_rows, dtype=jnp.int32)
        scores = jnp.einsum('qhd,khd->hqk', query_block, key_heads, precision=lax.Precision.HIGHEST) * HEAD_DIM ** (-0.5)
        scores = low_back(scores)
        allowed = (key_pos[None, :] <= query_pos[:, None]) | (key_pos[None, :] < prefix)
        scores = jnp.where(allowed[None], scores, MASKED)
        probabilities = jax.nn.softmax(scores, axis=-1)
        return jnp.einsum('hqk,khd->qhd', low(probabilities), value_heads, precision=lax.Precision.HIGHEST)
    mixed = lax.map(one_block, (query_blocks, block_starts))
    return mixed.reshape(length, HEADS * HEAD_DIM)

def block_forward(inputs, params, prefix):
    attn_gain, mlp_gain, query_weight, key_weight, value_weight, out_weight, gate_weight, up_weight, down_weight = params
    length = inputs.shape[0]
    cos_table, sine_table = rope_tables(length)
    normed = low(norm_rows(inputs, low(attn_gain)))

    def head_split(matrix):
        return low_back(matmul_high(normed, low(matrix))).reshape(length, HEADS, HEAD_DIM)

    def rotary(values):
        return values * cos_table[:, None] + rotate(values) * sine_table[:, None]
    queries = low(rotary(head_split(query_weight)))
    key_heads = low(rotary(head_split(key_weight)))
    value_heads = low(head_split(value_weight))
    mixed_low = low(low_back(attention(queries, key_heads, value_heads, prefix)))
    hidden = inputs + low_back(matmul_high(mixed_low, low(out_weight)))
    hnorm = low(norm_rows(hidden, low(mlp_gain)))
    gate_out = low_back(matmul_high(hnorm, low(gate_weight)))
    up_out = low_back(matmul_high(hnorm, low(up_weight)))
    activated = low(jax.nn.silu(gate_out) * up_out)
    return hidden + low_back(matmul_high(activated, low(down_weight)))

def reference(layer_input, output_cotangent, prefix_len, attn_gain, mlp_gain, query_weight, key_weight, value_weight, out_weight, gate_weight, up_weight, down_weight):
    params = (attn_gain, mlp_gain, query_weight, key_weight, value_weight, out_weight, gate_weight, up_weight, down_weight)

    def one_sequence(totals, element):
        seq_rows, seq_grad, prefix = element
        layer_out, pullback = jax.vjp(lambda inputs, weights: block_forward(inputs, weights, prefix), seq_rows.astype(jnp.float32), params)
        input_back, param_back = pullback(seq_grad.astype(jnp.float32))
        totals = jax.tree.map(lambda left, right: left + right, totals, param_back)
        return (totals, (layer_out.astype(jnp.bfloat16), input_back.astype(jnp.bfloat16)))
    zero_grads = jax.tree.map(jnp.zeros_like, params)
    totals, (outputs, input_grads) = lax.scan(one_sequence, zero_grads, (jnp.swapaxes(layer_input, 0, 1), jnp.swapaxes(output_cotangent, 0, 1), prefix_len))
    return (jnp.swapaxes(outputs, 0, 1), jnp.swapaxes(input_grads, 0, 1), totals[0], totals[1], totals[2], totals[3], totals[4], totals[5], totals[6], totals[7], totals[8])
```

```python
import functools
import math

import jax
import jax.numpy as jnp
from jax import lax
from jax.experimental import pallas as pl
from jax.experimental.pallas import tpu as pltpu
from jax.sharding import PartitionSpec as P

HEAD_DIM = 64


EPS = 1e-06
BASE = 10000.0
MASKED = -1e30


def partner(block, axis, apart):
    count = lax.axis_size(axis)
    route = []
    for low in range(count):
        high = low | 1 << apart
        if high != low and high < count:
            route += [(low, high), (high, low)]
    return lax.ppermute(block, axis, route)


def from_behind(value, axis, steps):
    count = lax.axis_size(axis)
    pairs = [(source, (source + steps) % count) for source in range(count)]
    return lax.ppermute(value, axis, pairs)


def norm_rows(values, gain):
    return values * lax.rsqrt(jnp.mean(values * values, axis=-1, keepdims=True) + EPS) * gain


def rope_tables(positions):
    half_dim = HEAD_DIM // 2
    frequency = jnp.exp(
        jnp.arange(half_dim, dtype=jnp.float32) * (-2.0 * math.log(BASE) / HEAD_DIM)
    )
    angles = positions.astype(jnp.float32)[:, None] * frequency[None, :]
    cos_table = jnp.concatenate([jnp.cos(angles), jnp.cos(angles)], axis=1)
    sine_table = jnp.concatenate([jnp.sin(angles), jnp.sin(angles)], axis=1)
    return (cos_table[:, None, None, :], sine_table[:, None, None, :])


def rotary(values, cos_table, sine_table):
    half_dim = values.shape[-1] // 2
    turned = jnp.concatenate([-values[..., half_dim:], values[..., :half_dim]], axis=-1)
    return values * cos_table + turned * sine_table


def unrotary(grads, cos_table, sine_table):
    half_dim = grads.shape[-1] // 2
    scaled = grads * sine_table
    turned = jnp.concatenate([scaled[..., half_dim:], -scaled[..., :half_dim]], axis=-1)
    return grads * cos_table + turned


def block_positions(device, block_len, ctx_size):
    half_len = block_len // 2
    steps = jnp.arange(half_len, dtype=jnp.int32)
    first_part = 2 * device * half_len + steps
    second_part = (2 * ctx_size - 1 - 2 * device) * half_len + steps
    return jnp.concatenate([first_part, second_part], axis=0)


def mirror_rows(values):
    ctx_bits = lax.axis_size("ctx").bit_length() - 1
    for bit in range(ctx_bits):
        values = partner(values, "ctx", bit)
    return values


def visible(prefix_len, query_pos, key_pos):
    causal = key_pos[None, :] <= query_pos[:, None]
    opened = key_pos[None, None, :] < prefix_len[:, None, None]
    return (causal[None] | opened)[:, None]


def block_needed(prefix_len, query_pos, key_pos):
    first_key = jnp.min(key_pos)
    return (first_key <= jnp.max(query_pos)) | jnp.any(prefix_len > first_key)


def attend_step(softmax_state, queries, key_value, prefix_len, query_pos, key_pos):
    key_heads = key_value[..., :HEAD_DIM]
    value_heads = key_value[..., HEAD_DIM:]

    def compute(state_in):
        row_max, row_sum, weighted = state_in
        scores = jnp.einsum(
            "qshd,kshd->shqk", queries, key_heads, preferred_element_type=jnp.float32
        ) * HEAD_DIM ** (-0.5)
        allowed = visible(prefix_len, query_pos, key_pos)
        block_max = jnp.max(jnp.where(allowed, scores, MASKED), axis=-1)
        fresh_max = jnp.maximum(row_max, block_max)
        exps = jnp.where(allowed, jnp.exp(scores - fresh_max[..., None]), 0.0)
        factor = jnp.exp(row_max - fresh_max)
        row_sum = row_sum * factor + jnp.sum(exps, axis=-1)
        weighted = weighted * jnp.transpose(factor, (2, 0, 1))[..., None] + jnp.einsum(
            "shqk,kshd->qshd",
            exps.astype(jnp.bfloat16),
            value_heads,
            preferred_element_type=jnp.float32,
        )
        return (fresh_max, row_sum, weighted)

    def skipped(state_in):
        return state_in

    return lax.cond(block_needed(prefix_len, query_pos, key_pos), compute, skipped, softmax_state)


def attend_back(
    queries, attn_grad, log_total, delta_rows, key_value, prefix_len, query_pos, key_pos
):
    key_heads = key_value[..., :HEAD_DIM]
    value_heads = key_value[..., HEAD_DIM:]
    score_scale = HEAD_DIM ** (-0.5)

    def compute(unused):
        scores = (
            jnp.einsum("qshd,kshd->shqk", queries, key_heads, preferred_element_type=jnp.float32)
            * score_scale
        )
        allowed = visible(prefix_len, query_pos, key_pos)
        probabilities = jnp.where(allowed, jnp.exp(scores - log_total[..., None]), 0.0)
        prob_grad = jnp.einsum(
            "qshd,kshd->shqk", attn_grad, value_heads, preferred_element_type=jnp.float32
        )
        score_grad = (probabilities * (prob_grad - delta_rows[..., None])).astype(jnp.bfloat16)
        query_part = (
            jnp.einsum("shqk,kshd->qshd", score_grad, key_heads, preferred_element_type=jnp.float32)
            * score_scale
        )
        key_part = (
            jnp.einsum("shqk,qshd->kshd", score_grad, queries, preferred_element_type=jnp.float32)
            * score_scale
        )
        value_part = jnp.einsum(
            "shqk,qshd->kshd",
            probabilities.astype(jnp.bfloat16),
            attn_grad,
            preferred_element_type=jnp.float32,
        )
        return (query_part, jnp.concatenate([key_part, value_part], axis=-1))

    def skipped(unused):
        return (jnp.zeros(queries.shape, jnp.float32), jnp.zeros(key_value.shape, jnp.float32))

    return lax.cond(block_needed(prefix_len, query_pos, key_pos), compute, skipped, 0)


def pass_grads(key_grads):
    return from_behind(key_grads.astype(jnp.bfloat16), "ctx", 1).astype(key_grads.dtype)


def body(
    layer_input,
    output_cotangent,
    prefix_len,
    attn_gain,
    mlp_gain,
    query_weight,
    key_weight,
    value_weight,
    out_weight,
    gate_weight,
    up_weight,
    down_weight,
):
    block_len, seq_count, width = layer_input.shape
    half_len = block_len // 2
    ctx_size = lax.axis_size("ctx")
    ctx_index = lax.axis_index("ctx")
    moved = mirror_rows(jnp.stack([layer_input[half_len:], output_cotangent[half_len:]], axis=0))
    layer_input = jnp.concatenate([layer_input[:half_len], moved[0]], axis=0)
    output_cotangent = jnp.concatenate([output_cotangent[:half_len], moved[1]], axis=0)
    query_pos = block_positions(ctx_index, block_len, ctx_size)
    cos_table, sine_table = rope_tables(query_pos)
    gain_one, full_query, full_key, full_value, full_out = (
        lax.all_gather(attn_gain.astype(jnp.bfloat16), "fsdp", axis=0, tiled=True),
        lax.all_gather(query_weight.astype(jnp.bfloat16), "fsdp", axis=0, tiled=True),
        lax.all_gather(key_weight.astype(jnp.bfloat16), "fsdp", axis=0, tiled=True),
        lax.all_gather(value_weight.astype(jnp.bfloat16), "fsdp", axis=0, tiled=True),
        lax.all_gather(out_weight.astype(jnp.bfloat16), "fsdp", axis=1, tiled=True),
    )
    gain_two, full_gate, full_up, full_down = (
        lax.all_gather(mlp_gain.astype(jnp.bfloat16), "fsdp", axis=0, tiled=True),
        lax.all_gather(gate_weight.astype(jnp.bfloat16), "fsdp", axis=0, tiled=True),
        lax.all_gather(up_weight.astype(jnp.bfloat16), "fsdp", axis=0, tiled=True),
        lax.all_gather(down_weight.astype(jnp.bfloat16), "fsdp", axis=1, tiled=True),
    )
    heads_local = full_query.shape[1] // HEAD_DIM
    inputs = layer_input.astype(jnp.float32)
    attn_scale = gain_one.astype(jnp.float32)
    normed_low = norm_rows(inputs, attn_scale).astype(jnp.bfloat16)

    def project(matrix):
        product = jnp.einsum("bsd,de->bse", normed_low, matrix, preferred_element_type=jnp.float32)
        return product.reshape(block_len, seq_count, heads_local, HEAD_DIM)

    queries = rotary(project(full_query), cos_table, sine_table).astype(jnp.bfloat16)
    key_heads = rotary(project(full_key), cos_table, sine_table).astype(jnp.bfloat16)
    value_heads = project(full_value).astype(jnp.bfloat16)
    key_value = jnp.concatenate([key_heads, value_heads], axis=-1)
    stats_shape = (seq_count, heads_local, block_len)
    initial = (
        jnp.full(stats_shape, MASKED, jnp.float32),
        jnp.zeros(stats_shape, jnp.float32),
        jnp.zeros((block_len, seq_count, heads_local, HEAD_DIM), jnp.float32),
    )
    softmax_state = attend_step(initial, queries, key_value, prefix_len, query_pos, query_pos)

    def forward_shift(counter, loop_carry):
        state_in, moving = loop_carry
        moving = from_behind(moving, "ctx", 1)
        source = (ctx_index - counter) % ctx_size
        key_pos = block_positions(source, block_len, ctx_size)
        state_in = attend_step(state_in, queries, moving, prefix_len, query_pos, key_pos)
        return (state_in, moving)

    softmax_state, unused_keys = lax.fori_loop(
        1, ctx_size, forward_shift, (softmax_state, key_value)
    )
    row_max, row_sum, weighted = softmax_state
    log_total = row_max + jnp.log(row_sum)
    attn_exact = weighted / jnp.transpose(row_sum, (2, 0, 1))[..., None]
    mixed_low = attn_exact.reshape(block_len, seq_count, heads_local * HEAD_DIM).astype(
        jnp.bfloat16
    )
    attn_part = jnp.einsum("bse,ed->bsd", mixed_low, full_out, preferred_element_type=jnp.float32)
    hidden = inputs + lax.psum(attn_part.astype(jnp.bfloat16), "tp").astype(jnp.float32)
    mlp_scale = gain_two.astype(jnp.float32)
    hnorm_low = norm_rows(hidden, mlp_scale).astype(jnp.bfloat16)
    gate_out = jnp.einsum("bsd,df->bsf", hnorm_low, full_gate, preferred_element_type=jnp.float32)
    up_out = jnp.einsum("bsd,df->bsf", hnorm_low, full_up, preferred_element_type=jnp.float32)
    activated = (jax.nn.silu(gate_out) * up_out).astype(jnp.bfloat16)
    down_part = jnp.einsum("bsf,fd->bsd", activated, full_down, preferred_element_type=jnp.float32)
    result = hidden + lax.psum(down_part.astype(jnp.bfloat16), "tp").astype(jnp.float32)
    layer_output = result.astype(jnp.bfloat16)
    grad_float = output_cotangent.astype(jnp.float32)
    down_w_grad = jnp.einsum(
        "bsf,bsd->fd", activated, output_cotangent, preferred_element_type=jnp.float32
    )
    act_grad = jnp.einsum(
        "bsd,fd->bsf", output_cotangent, full_down, preferred_element_type=jnp.float32
    )
    unused_value, silu_pullback = jax.vjp(
        lambda gate_in, up_in: jax.nn.silu(gate_in) * up_in, gate_out, up_out
    )
    gate_back, up_back = silu_pullback(act_grad)
    gate_grad = gate_back.astype(jnp.bfloat16)
    up_grad = up_back.astype(jnp.bfloat16)
    gate_w_grad = jnp.einsum(
        "bsd,bsf->df", hnorm_low, gate_grad, preferred_element_type=jnp.float32
    )
    up_w_grad = jnp.einsum("bsd,bsf->df", hnorm_low, up_grad, preferred_element_type=jnp.float32)
    hnorm_part = jnp.einsum(
        "bsf,df->bsd", gate_grad, full_gate, preferred_element_type=jnp.float32
    ) + jnp.einsum("bsf,df->bsd", up_grad, full_up, preferred_element_type=jnp.float32)
    hnorm_grad = lax.psum(hnorm_part.astype(jnp.bfloat16), "tp").astype(jnp.float32)
    unused_norm, norm_pullback = jax.vjp(norm_rows, hidden, mlp_scale)
    hidden_back, mlp_gain_part = norm_pullback(hnorm_grad)
    hidden_grad = grad_float + hidden_back
    hidden_low = hidden_grad.astype(jnp.bfloat16)
    out_w_grad = jnp.einsum(
        "bse,bsd->ed", mixed_low, hidden_low, preferred_element_type=jnp.float32
    )
    attn_grad = jnp.einsum(
        "bsd,ed->bse", hidden_low, full_out, preferred_element_type=jnp.float32
    ).astype(jnp.bfloat16)
    attn_grad = attn_grad.reshape(block_len, seq_count, heads_local, HEAD_DIM)
    delta_rows = jnp.transpose(
        jnp.sum(attn_grad.astype(jnp.float32) * attn_exact, axis=-1), (1, 2, 0)
    )
    zero_query = jnp.zeros((block_len, seq_count, heads_local, HEAD_DIM), jnp.float32)

    def backward_shift(counter, loop_carry):
        query_acc, moving, travelling = loop_carry
        source = (ctx_index - counter) % ctx_size
        key_pos = block_positions(source, block_len, ctx_size)
        query_part, key_part = attend_back(
            queries, attn_grad, log_total, delta_rows, moving, prefix_len, query_pos, key_pos
        )
        travelling = pass_grads(travelling + key_part)
        moving = from_behind(moving, "ctx", 1)
        return (query_acc + query_part, moving, travelling)

    travel_zero = jnp.zeros((block_len, seq_count, heads_local, 2 * HEAD_DIM), jnp.float32)
    query_acc, moving, travelling = lax.fori_loop(
        0, ctx_size - 1, backward_shift, (zero_query, key_value, travel_zero)
    )
    last_source = (ctx_index + 1) % ctx_size
    last_pos = block_positions(last_source, block_len, ctx_size)
    query_part, key_part = attend_back(
        queries, attn_grad, log_total, delta_rows, moving, prefix_len, query_pos, last_pos
    )
    query_acc = query_acc + query_part
    own_grads = pass_grads(travelling + key_part)
    flat_shape = (block_len, seq_count, heads_local * HEAD_DIM)
    query_grad = unrotary(query_acc, cos_table, sine_table).astype(jnp.bfloat16).reshape(flat_shape)
    key_grad = (
        unrotary(own_grads[..., :HEAD_DIM], cos_table, sine_table)
        .astype(jnp.bfloat16)
        .reshape(flat_shape)
    )
    value_grad = own_grads[..., HEAD_DIM:].astype(jnp.bfloat16).reshape(flat_shape)
    query_w_grad = jnp.einsum(
        "bsd,bse->de", normed_low, query_grad, preferred_element_type=jnp.float32
    )
    key_w_grad = jnp.einsum("bsd,bse->de", normed_low, key_grad, preferred_element_type=jnp.float32)
    value_w_grad = jnp.einsum(
        "bsd,bse->de", normed_low, value_grad, preferred_element_type=jnp.float32
    )
    normed_part = (
        jnp.einsum("bse,de->bsd", query_grad, full_query, preferred_element_type=jnp.float32)
        + jnp.einsum("bse,de->bsd", key_grad, full_key, preferred_element_type=jnp.float32)
        + jnp.einsum("bse,de->bsd", value_grad, full_value, preferred_element_type=jnp.float32)
    )
    normed_grad = lax.psum(normed_part.astype(jnp.bfloat16), "tp").astype(jnp.float32)
    unused_first, first_pullback = jax.vjp(norm_rows, inputs, attn_scale)
    input_back, attn_gain_part = first_pullback(normed_grad)
    input_grad = (hidden_grad + input_back).astype(jnp.bfloat16)
    returned = mirror_rows(jnp.stack([layer_output[half_len:], input_grad[half_len:]], axis=0))
    layer_output = jnp.concatenate([layer_output[:half_len], returned[0]], axis=0)
    input_grad = jnp.concatenate([input_grad[:half_len], returned[1]], axis=0)
    shards = (
        lax.psum_scatter(
            attn_gain_part.astype(jnp.bfloat16), "fsdp", scatter_dimension=0, tiled=True
        ).astype(jnp.float32),
        lax.psum_scatter(
            mlp_gain_part.astype(jnp.bfloat16), "fsdp", scatter_dimension=0, tiled=True
        ).astype(jnp.float32),
        lax.psum_scatter(
            query_w_grad.astype(jnp.bfloat16), "fsdp", scatter_dimension=0, tiled=True
        ).astype(jnp.float32),
        lax.psum_scatter(
            key_w_grad.astype(jnp.bfloat16), "fsdp", scatter_dimension=0, tiled=True
        ).astype(jnp.float32),
        lax.psum_scatter(
            value_w_grad.astype(jnp.bfloat16), "fsdp", scatter_dimension=0, tiled=True
        ).astype(jnp.float32),
        lax.psum_scatter(
            out_w_grad.astype(jnp.bfloat16), "fsdp", scatter_dimension=1, tiled=True
        ).astype(jnp.float32),
        lax.psum_scatter(
            gate_w_grad.astype(jnp.bfloat16), "fsdp", scatter_dimension=0, tiled=True
        ).astype(jnp.float32),
        lax.psum_scatter(
            up_w_grad.astype(jnp.bfloat16), "fsdp", scatter_dimension=0, tiled=True
        ).astype(jnp.float32),
        lax.psum_scatter(
            down_w_grad.astype(jnp.bfloat16), "fsdp", scatter_dimension=1, tiled=True
        ).astype(jnp.float32),
    )
    totals = (
        lax.psum(shards[0].astype(jnp.bfloat16), "ctx").astype(jnp.float32),
        lax.psum(shards[1].astype(jnp.bfloat16), "ctx").astype(jnp.float32),
        lax.psum(shards[2].astype(jnp.bfloat16), "ctx").astype(jnp.float32),
        lax.psum(shards[3].astype(jnp.bfloat16), "ctx").astype(jnp.float32),
        lax.psum(shards[4].astype(jnp.bfloat16), "ctx").astype(jnp.float32),
        lax.psum(shards[5].astype(jnp.bfloat16), "ctx").astype(jnp.float32),
        lax.psum(shards[6].astype(jnp.bfloat16), "ctx").astype(jnp.float32),
        lax.psum(shards[7].astype(jnp.bfloat16), "ctx").astype(jnp.float32),
        lax.psum(shards[8].astype(jnp.bfloat16), "ctx").astype(jnp.float32),
    )
    return (
        layer_output,
        input_grad,
        totals[0],
        totals[1],
        totals[2],
        totals[3],
        totals[4],
        totals[5],
        totals[6],
        totals[7],
        totals[8],
    )


MESH = pl.DeviceIdType.MESH
VMEM_LIMIT = 60 << 20


def place():
    ctx = lax.axis_index("ctx")
    along_x = ctx + 1 - 2 * lax.rem(ctx, 2)
    along_y = lax.rem(ctx + 2, 4)
    return lax.axis_index("fsdp"), ctx, along_x, along_y, 3 - ctx


def greet(devices):
    barrier = pltpu.get_barrier_semaphore()
    for device in devices:
        pl.semaphore_signal(barrier, inc=1, device_id=device, device_id_type=MESH)
    pl.semaphore_wait(barrier, len(devices))


def rows_at(block, rows):
    return pl.ds(pl.multiple_of(block * rows, 16), rows)


def send(source, target, send_sem, recv_sem, device):
    return pltpu.make_async_remote_copy(
        src_ref=source,
        dst_ref=target,
        send_sem=send_sem,
        recv_sem=recv_sem,
        device_id=device,
        device_id_type=MESH,
    )


def column_chunks(shapes, widest):
    chunks = []
    for index, (rows, columns) in enumerate(shapes):
        count = -(-columns // widest)
        while columns % count or (columns // count) % 128:
            count += 1
        width = columns // count
        chunks += [(index, rows // 4, part * width, width) for part in range(count)]
    return [chunk + (number % 2,) for number, chunk in enumerate(chunks)]


def gather_steps(chunks, shard_refs, full_refs, local_sem, send_sems, recv_sems):
    fsdp, ctx, along_x, along_y, across = place()
    last = lax.axis_size("fsdp") - 1

    def region(chunk, shard, quarter):
        index, rows, low, width, _ = chunk
        return full_refs[index].at[rows_at(shard * 4 + quarter, rows), pl.ds(low, width)]

    def pass_on(number, shard, quarter, kind, device, source=None):
        target = region(chunks[number], shard, quarter)
        return send(
            target if source is None else source,
            target,
            send_sems.at[number, shard, kind],
            recv_sems.at[number, shard, quarter],
            device,
        )

    def own_source(number):
        index, rows, low, width, _ = chunks[number]
        return shard_refs[index].at[rows_at(ctx, rows), pl.ds(low, width)]

    def arrived(number, shard, quarter):
        pass_on(number, shard, quarter, 0, {"ctx": along_x}).wait_recv()

    count = range(len(chunks))
    up, down = {"fsdp": lax.rem(fsdp + 1, last + 1)}, {"fsdp": lax.rem(fsdp + last, last + 1)}
    to_x, to_y = {"ctx": along_x}, {"ctx": along_y}

    def begin():
        for number in count:

            @pl.when(fsdp < last)
            def _(number=number):
                pass_on(number, fsdp, ctx, 0, up, own_source(number)).start()

            @pl.when(fsdp > 0)
            def _(number=number):
                pass_on(number, fsdp, ctx, 1, down, own_source(number)).start()

        for index, shard_ref in enumerate(shard_refs):
            rows = shard_ref.shape[0]
            pltpu.make_async_copy(
                shard_ref, full_refs[index].at[rows_at(fsdp, rows)], local_sem.at[index]
            ).start()

    def each(steps, act):
        for sign in (-1, 1):
            shard = fsdp + sign * steps

            @pl.when((shard >= 0) & (shard <= last))
            def _(sign=sign, shard=shard):
                act(shard, sign)

    def from_line(number, steps):
        def act(shard, sign):
            arrived(number, shard, ctx)
            if sign < 0:

                @pl.when(fsdp < last)
                def _():
                    pass_on(number, shard, ctx, 0, up).start()

            else:

                @pl.when(fsdp > 0)
                def _():
                    pass_on(number, shard, ctx, 1, down).start()

            pass_on(number, shard, ctx, 2, to_x).start()
            pass_on(number, shard, ctx, 3, to_y).start()

        each(steps, act)

    def to_corner(number, steps):
        def act(shard, sign):
            if chunks[number][-1] == 0:
                arrived(number, shard, along_x)
                pass_on(number, shard, along_x, 4, to_y).start()
            else:
                arrived(number, shard, along_y)
                pass_on(number, shard, along_y, 4, to_x).start()

        each(steps, act)

    def finish():
        for steps in range(1, last + 1):
            for number in count:

                def act(shard, sign, number=number):
                    arrived(number, shard, along_y if chunks[number][-1] == 0 else along_x)
                    arrived(number, shard, across)
                    forward = fsdp < last if sign < 0 else fsdp > 0

                    @pl.when(forward)
                    def _():
                        pass_on(number, shard, ctx, 0 if sign < 0 else 1, up).wait_send()

                    for kind in (2, 3, 4):
                        pass_on(number, shard, ctx, kind, to_x).wait_send()

                each(steps, act)
        for number in count:

            @pl.when(fsdp < last)
            def _(number=number):
                pass_on(number, fsdp, ctx, 0, up, own_source(number)).wait_send()

            @pl.when(fsdp > 0)
            def _(number=number):
                pass_on(number, fsdp, ctx, 1, down, own_source(number)).wait_send()

        for index, shard_ref in enumerate(shard_refs):
            rows = shard_ref.shape[0]
            pltpu.make_async_copy(
                shard_ref, full_refs[index].at[rows_at(fsdp, rows)], local_sem.at[index]
            ).wait()

    return begin, from_line, to_corner, finish


def neighbours(fsdp, along_x, along_y):
    size = lax.axis_size("fsdp")
    return [
        {"ctx": along_x},
        {"ctx": along_y},
        {"fsdp": lax.rem(fsdp + 1, size)},
        {"fsdp": lax.rem(fsdp + size - 1, size)},
    ]


def gather_kernel(chunks, arrays, *refs):
    shard_refs, full_refs = refs[:arrays], refs[arrays : 2 * arrays]
    local_sem, send_sems, recv_sems = refs[2 * arrays :]
    fsdp, ctx, along_x, along_y, across = place()
    greet(neighbours(fsdp, along_x, along_y))
    begin, from_line, to_corner, finish = gather_steps(
        chunks, shard_refs, full_refs, local_sem, send_sems, recv_sems
    )
    begin()
    last = lax.axis_size("fsdp") - 1
    for steps in range(1, last + 2):
        for number in range(len(chunks)):
            if steps <= last:
                from_line(number, steps)
            if steps > 1:
                to_corner(number, steps - 1)
    finish()


def gather_scratch(shards, chunks):
    return [
        pltpu.SemaphoreType.DMA((len(shards),)),
        pltpu.SemaphoreType.DMA((len(chunks), 4, 5)),
        pltpu.SemaphoreType.DMA((len(chunks), 4, 4)),
    ]


def gather_shards(shards, collective_id):
    chunks = column_chunks([shard.shape for shard in shards], 512)
    size = lax.axis_size("fsdp")
    anywhere = pl.BlockSpec(memory_space=pl.ANY)
    return pl.pallas_call(
        functools.partial(gather_kernel, chunks, len(shards)),
        out_shape=[
            jax.ShapeDtypeStruct((size * shard.shape[0], shard.shape[1]), shard.dtype)
            for shard in shards
        ],
        in_specs=[pl.BlockSpec(memory_space=pltpu.VMEM)] * len(shards),
        out_specs=[anywhere] * len(shards),
        scratch_shapes=gather_scratch(shards, chunks),
        compiler_params=pltpu.CompilerParams(
            collective_id=collective_id, has_side_effects=True, vmem_limit_bytes=VMEM_LIMIT
        ),
        name="gather_shards",
    )(*shards)


def reduce_kernel(chunks, arrays, *refs):
    full_refs, out_refs = refs[:arrays], refs[arrays : 2 * arrays]
    rest = refs[2 * arrays :]
    count = len(chunks)
    buffers = [rest[6 * number : 6 * number + 6] for number in range(count)]
    load_sems, send_sems, recv_sems = rest[6 * count :]
    fsdp, ctx, along_x, along_y, across = place()
    size = lax.axis_size("fsdp")
    others = [{"fsdp": lax.rem(fsdp + step, size)} for step in range(1, size)]
    greet([{"ctx": along_x}, {"ctx": along_y}] + others)

    def quarter_of(number, quarter):
        index, rows, low, width, _ = chunks[number]
        return full_refs[index].at[:, rows_at(quarter, rows), pl.ds(low, width)]

    def result(number, quarter):
        index, rows, low, width, _ = chunks[number]
        return out_refs[index].at[rows_at(quarter, rows), pl.ds(low, width)]

    def first_second(number):
        return (along_x, along_y) if chunks[number][-1] == 0 else (along_y, along_x)

    def exchange(number, part):
        first, _ = first_second(number)
        return send(
            quarter_of(number, first if part == 0 else across),
            buffers[number][1].at[part],
            send_sems.at[number, part],
            recv_sems.at[number, part],
            {"ctx": first},
        )

    def load(number, part):
        _, second = first_second(number)
        return pltpu.make_async_copy(
            quarter_of(number, ctx if part == 0 else second),
            buffers[number][0].at[part],
            load_sems.at[number, part],
        )

    def second_hop(number):
        _, second = first_second(number)
        return send(
            buffers[number][2],
            buffers[number][3],
            send_sems.at[number, 2],
            recv_sems.at[number, 2],
            {"ctx": second},
        )

    def along_line(number, step):
        return send(
            buffers[number][4].at[lax.rem(fsdp + step, size)],
            buffers[number][5].at[step - 1],
            send_sems.at[number, 2 + step],
            recv_sems.at[number, 2 + step],
            others[step - 1],
        )

    def spread(number, quarter, kind, target):
        place_there = result(number, quarter)
        return send(
            place_there,
            place_there,
            send_sems.at[number, 2 + size + kind],
            recv_sems.at[number, 2 + size + kind],
            {"ctx": target},
        )

    def stage(number, at):
        first, second = first_second(number)
        own, landed, passing, arrived, total, line = buffers[number]
        if at == 0:
            for part in (1, 0):
                exchange(number, part).start()
                load(number, part).start()
        elif at == 1:
            load(number, 1).wait()
            exchange(number, 1).wait_recv()
            passing[...] = (own[1].astype(jnp.float32) + landed[1].astype(jnp.float32)).astype(
                jnp.bfloat16
            )
            second_hop(number).start()
        elif at == 2:
            load(number, 0).wait()
            exchange(number, 0).wait_recv()
            second_hop(number).wait_recv()
            total[...] = (
                own[0].astype(jnp.float32)
                + landed[0].astype(jnp.float32)
                + arrived[...].astype(jnp.float32)
            ).astype(jnp.bfloat16)
            for step in range(1, size):
                along_line(number, step).start()
        elif at == 3:
            value = total[fsdp].astype(jnp.float32)
            for step in range(1, size):
                along_line(number, step).wait_recv()
                value = value + line[step - 1].astype(jnp.float32)
            index, rows, low, width, _ = chunks[number]
            out_refs[index][rows_at(ctx, rows), pl.ds(low, width)] = value.astype(jnp.bfloat16)
            spread(number, ctx, 0, first).start()
            spread(number, ctx, 1, second).start()
        elif at == 4:
            spread(number, first, 0, first).wait_recv()
            spread(number, first, 2, second).start()
        else:
            spread(number, second, 1, second).wait_recv()
            spread(number, across, 2, second).wait_recv()
            for part in (0, 1):
                exchange(number, part).wait_send()
            second_hop(number).wait_send()
            for step in range(1, size):
                along_line(number, step).wait_send()
            for kind in range(3):
                spread(number, ctx, kind, first).wait_send()

    for number in range(count):
        stage(number, 0)
    lag = 2
    for tick in range(count + 4 * lag):
        for at in range(5, 0, -1):
            number = tick - (at - 1) * lag
            if 0 <= number < count:
                stage(number, at)


def reduce_grads(grads, collective_id):
    size = lax.axis_size("fsdp")
    shapes = [(grad.shape[0] // size, grad.shape[1]) for grad in grads]
    chunks = column_chunks(shapes, 512)
    anywhere = pl.BlockSpec(memory_space=pl.ANY)
    scratch = []
    for _, rows, _, width, _ in chunks:
        block = (size, rows, width)
        for shape in ((2,) + block, (2,) + block, block, block, block, (size - 1, rows, width)):
            scratch.append(pltpu.VMEM(shape, jnp.bfloat16))
    scratch += [
        pltpu.SemaphoreType.DMA((len(chunks), 2)),
        pltpu.SemaphoreType.DMA((len(chunks), size + 5)),
        pltpu.SemaphoreType.DMA((len(chunks), size + 5)),
    ]
    return pl.pallas_call(
        functools.partial(reduce_kernel, chunks, len(grads)),
        out_shape=[jax.ShapeDtypeStruct(shape, jnp.bfloat16) for shape in shapes],
        in_specs=[anywhere] * len(grads),
        out_specs=[pl.BlockSpec(memory_space=pltpu.VMEM)] * len(grads),
        scratch_shapes=scratch,
        compiler_params=pltpu.CompilerParams(
            collective_id=collective_id, has_side_effects=True, vmem_limit_bytes=VMEM_LIMIT
        ),
        name="reduce_grads",
    )(*[grad.reshape(size, shape[0], shape[1]) for grad, shape in zip(grads, shapes)])


def swap_kernel(arrays, *refs):
    block_refs, out_ref = refs[:arrays], refs[arrays]
    local_sems, send_sems, recv_sems = refs[arrays + 1 :]
    fsdp, ctx, along_x, along_y, across = place()
    targets = (across, along_x, along_y)
    greet([{"ctx": target} for target in targets])
    copies = []
    for index, block_ref in enumerate(block_refs):
        for number, target in enumerate(targets):
            copy = send(
                block_ref.at[target],
                out_ref.at[index, ctx],
                send_sems.at[index, number],
                recv_sems.at[index, number],
                {"ctx": target},
            )
            copy.start()
            copies.append(copy)
        copy = pltpu.make_async_copy(
            block_ref.at[ctx], out_ref.at[index, ctx], local_sems.at[index]
        )
        copy.start()
        copies.append(copy)
    for copy in copies:
        copy.wait()


def swap_blocks(blocks, collective_id):
    arrays = len(blocks)
    return pl.pallas_call(
        functools.partial(swap_kernel, arrays),
        out_shape=jax.ShapeDtypeStruct((arrays,) + blocks[0].shape, blocks[0].dtype),
        in_specs=[pl.BlockSpec(memory_space=pltpu.VMEM)] * arrays,
        out_specs=pl.BlockSpec(memory_space=pl.ANY),
        scratch_shapes=[
            pltpu.SemaphoreType.DMA((arrays,)),
            pltpu.SemaphoreType.DMA((arrays, 3)),
            pltpu.SemaphoreType.DMA((arrays, 3)),
        ],
        compiler_params=pltpu.CompilerParams(
            collective_id=collective_id, has_side_effects=True, vmem_limit_bytes=VMEM_LIMIT
        ),
        name="swap_blocks",
    )(*blocks)


def dot(left, right):
    return jnp.dot(left, right, preferred_element_type=jnp.float32)


def turn(block):
    return block.astype(jnp.float32).T.astype(block.dtype)


def seen(prefix, row_block, key_block, rows, keys, values, fill):
    if (key_block + 1) * keys <= row_block * rows + 1:
        return values
    key_pos = key_block * keys + lax.broadcasted_iota(jnp.int32, values.shape, 1)
    row_pos = row_block * rows + lax.broadcasted_iota(jnp.int32, values.shape, 0)
    allowed = key_pos < jnp.maximum(row_pos + 1, prefix)
    return jnp.where(allowed, values, fill)


def key_blocks(row_block, rows, keys, length):
    farthest = max((row_block + 1) * rows, length // 2)
    return range(-(-farthest // keys))


def attend_kernel(rows, prefix_ref, blocks_ref, mixed_ref, log_ref, query_ref, value_ref):
    places, keys = blocks_ref.shape[1], blocks_ref.shape[3]
    length = places * keys
    prefix = prefix_ref[0]
    for block in range(places):
        span = pl.ds(block * keys, keys)
        query_ref[span, :] = turn(blocks_ref[0, block] * jnp.bfloat16(HEAD_DIM ** (-0.5)))
        value_ref[span, :] = turn(blocks_ref[2, block])
    for row_block in range(length // rows):
        span = pl.ds(row_block * rows, rows)
        queries = query_ref[span, :]
        scores = []
        for block in key_blocks(row_block, rows, keys, length):
            scores.append(
                seen(
                    prefix, row_block, block, rows, keys, dot(queries, blocks_ref[1, block]), MASKED
                )
            )
        row_max = functools.reduce(
            jnp.maximum, [jnp.max(part, axis=1, keepdims=True) for part in scores]
        )
        row_sum = jnp.zeros_like(row_max)
        mixed = jnp.zeros((rows, HEAD_DIM), jnp.float32)
        for block, part in enumerate(scores):
            exps = jnp.exp(part - row_max)
            row_sum = row_sum + jnp.sum(exps, axis=1, keepdims=True)
            mixed = mixed + dot(exps.astype(jnp.bfloat16), value_ref[pl.ds(block * keys, keys), :])
        log_ref[0, span, :] = row_max + jnp.log(row_sum)
        block, inside = divmod(row_block * rows, keys)
        mixed_ref[block, :, pl.ds(inside, rows)] = (mixed / row_sum).T.astype(jnp.bfloat16)


def attend(blocks, prefix):
    _, places, features, keys = blocks.shape
    heads = features // HEAD_DIM
    length = places * keys
    return pl.pallas_call(
        functools.partial(attend_kernel, min(256, keys)),
        grid=(heads,),
        out_shape=(
            jax.ShapeDtypeStruct((places, features, keys), jnp.bfloat16),
            jax.ShapeDtypeStruct((heads, length, 1), jnp.float32),
        ),
        in_specs=[
            pl.BlockSpec(memory_space=pltpu.SMEM),
            pl.BlockSpec((3, places, HEAD_DIM, keys), lambda head: (0, 0, head, 0)),
        ],
        out_specs=(
            pl.BlockSpec((places, HEAD_DIM, keys), lambda head: (0, head, 0)),
            pl.BlockSpec((1, length, 1), lambda head: (head, 0, 0)),
        ),
        scratch_shapes=[
            pltpu.VMEM((length, HEAD_DIM), jnp.bfloat16),
            pltpu.VMEM((length, HEAD_DIM), jnp.bfloat16),
        ],
        compiler_params=pltpu.CompilerParams(vmem_limit_bytes=VMEM_LIMIT),
        name="attend",
    )(prefix, blocks)


def turn_back(grads, cos_table, sine_table):
    half = HEAD_DIM // 2
    low, high = grads[:half], grads[half:]
    return (
        low * cos_table + high * sine_table,
        high * cos_table - low * sine_table,
    )


def attend_back_kernel(
    rows,
    prefix_ref,
    blocks_ref,
    back_ref,
    log_ref,
    cos_ref,
    sine_ref,
    grads_ref,
    query_ref,
    key_ref,
    attn_ref,
    key_grad_ref,
    value_grad_ref,
):
    places, keys = blocks_ref.shape[1], blocks_ref.shape[3]
    length = places * keys
    half = HEAD_DIM // 2
    scale = HEAD_DIM ** (-0.5)
    prefix = prefix_ref[0]
    for block in range(places):
        span = pl.ds(block * keys, keys)
        query_ref[span, :] = turn(blocks_ref[0, block] * jnp.bfloat16(scale))
        key_ref[span, :] = turn(blocks_ref[1, block])
        attn_ref[span, :] = turn(back_ref[0, block])
    key_grad_ref[...] = jnp.zeros_like(key_grad_ref)
    value_grad_ref[...] = jnp.zeros_like(value_grad_ref)
    for row_block in range(length // rows):
        span = pl.ds(row_block * rows, rows)
        home, inside = divmod(row_block * rows, keys)
        lanes = pl.ds(inside, rows)
        queries, attn_grad = query_ref[span, :], attn_ref[span, :]
        queries_low = blocks_ref[0, home, :, lanes] * jnp.bfloat16(scale)
        attn_low = back_ref[0, home, :, lanes]
        total = log_ref[0, span, :]
        reach = key_blocks(row_block, rows, keys, length)
        weights, pulls = [], []
        delta = jnp.zeros((rows, 1), jnp.float32)
        for block in reach:
            part = dot(queries, blocks_ref[1, block])
            part = jnp.exp(seen(prefix, row_block, block, rows, keys, part, MASKED) - total)
            pull = dot(attn_grad, blocks_ref[2, block])
            delta = delta + jnp.sum(part * pull, axis=1, keepdims=True)
            weights.append(part)
            pulls.append(pull)
        query_grad = jnp.zeros((rows, HEAD_DIM), jnp.float32)
        for block in reach:
            key_span = pl.ds(block * keys, keys)
            score_grad = (weights[block] * (pulls[block] - delta)).astype(jnp.bfloat16)
            query_grad = query_grad + dot(score_grad, key_ref[key_span, :])
            key_grad_ref[:, key_span] += dot(queries_low, score_grad)
            value_grad_ref[:, key_span] += dot(attn_low, weights[block].astype(jnp.bfloat16))
        low, high = turn_back((query_grad * scale).T, cos_ref[:, span], sine_ref[:, span])
        grads_ref[0, home, :half, lanes] = low.astype(jnp.bfloat16)
        grads_ref[0, home, half:, lanes] = high.astype(jnp.bfloat16)
    for block in range(places):
        span = pl.ds(block * keys, keys)
        low, high = turn_back(key_grad_ref[:, span], cos_ref[:, span], sine_ref[:, span])
        grads_ref[1, block, :half] = low.astype(jnp.bfloat16)
        grads_ref[1, block, half:] = high.astype(jnp.bfloat16)
        grads_ref[2, block] = value_grad_ref[:, span].astype(jnp.bfloat16)


def attend_back_heads(blocks, back, log_total, prefix, cos_table, sine_table):
    _, places, features, keys = blocks.shape
    heads = features // HEAD_DIM
    length = places * keys
    whole = pl.BlockSpec(memory_space=pltpu.VMEM)
    return pl.pallas_call(
        functools.partial(attend_back_kernel, min(256, keys)),
        grid=(heads,),
        out_shape=jax.ShapeDtypeStruct(blocks.shape, jnp.bfloat16),
        in_specs=[
            pl.BlockSpec(memory_space=pltpu.SMEM),
            pl.BlockSpec((3, places, HEAD_DIM, keys), lambda head: (0, 0, head, 0)),
            pl.BlockSpec((1, places, HEAD_DIM, keys), lambda head: (0, 0, head, 0)),
            pl.BlockSpec((1, length, 1), lambda head: (head, 0, 0)),
            whole,
            whole,
        ],
        out_specs=pl.BlockSpec((3, places, HEAD_DIM, keys), lambda head: (0, 0, head, 0)),
        scratch_shapes=[
            pltpu.VMEM((length, HEAD_DIM), jnp.bfloat16),
            pltpu.VMEM((length, HEAD_DIM), jnp.bfloat16),
            pltpu.VMEM((length, HEAD_DIM), jnp.bfloat16),
            pltpu.VMEM((HEAD_DIM, length), jnp.float32),
            pltpu.VMEM((HEAD_DIM, length), jnp.float32),
        ],
        compiler_params=pltpu.CompilerParams(vmem_limit_bytes=VMEM_LIMIT),
        name="attend_back",
    )(prefix, blocks, back, log_total, cos_table, sine_table)


def both_cores(part):
    part = part.astype(jnp.bfloat16)
    size = lax.axis_size("tp")
    other = lax.ppermute(part, "tp", [(core, (core + 1) % size) for core in range(size)])
    return part.astype(jnp.float32) + other.astype(jnp.float32)


def matmul(spec, left, right):
    return jnp.einsum(spec, left, right, preferred_element_type=jnp.float32)


def half_tables(length):
    half = HEAD_DIM // 2
    frequency = jnp.exp(jnp.arange(half, dtype=jnp.float32) * (-2.0 * math.log(BASE) / HEAD_DIM))
    angles = frequency[:, None] * jnp.arange(length, dtype=jnp.float32)[None, :]
    return jnp.cos(angles), jnp.sin(angles)


def norm_back(values, gain, grads):
    scale = lax.rsqrt(jnp.mean(values * values, axis=-1, keepdims=True) + EPS)
    pulled = grads * gain
    inner = jnp.mean(values * pulled, axis=-1, keepdims=True)
    gain_part = jnp.sum(grads * values * scale, axis=(0, 1))
    return scale * pulled - values * (scale * scale * scale * inner), gain_part


def gains_in(first, second):
    both = jnp.stack([first.reshape(4, -1), second.reshape(4, -1)], axis=1)
    both = jnp.pad(both, ((0, 0), (0, 14), (0, 128 - both.shape[2])))
    return both.reshape(64, 128).astype(jnp.bfloat16)


def gains_out(packed, which, quarter):
    return packed.reshape(-1, 16, 128)[:, which, :quarter].reshape(-1)


def heads_body(
    layer_input,
    output_cotangent,
    prefix_len,
    attn_gain,
    mlp_gain,
    query_weight,
    key_weight,
    value_weight,
    out_weight,
    gate_weight,
    up_weight,
    down_weight,
):
    block_len, seq_count, width = layer_input.shape
    places = lax.axis_size("ctx")
    ctx_index = lax.axis_index("ctx")
    local = query_weight.shape[1]
    features = seq_count * local // places
    length = places * block_len
    quarter = attn_gain.shape[0] // 4
    low = jnp.bfloat16
    shards = [
        gains_in(attn_gain, mlp_gain),
        query_weight.astype(low),
        key_weight.astype(low),
        value_weight.astype(low),
        out_weight.T.astype(low),
        gate_weight.astype(low),
        up_weight.astype(low),
        down_weight.T.astype(low),
    ]
    gains, full_query, full_key, full_value, full_out, full_gate, full_up, full_down = (
        gather_shards(shards, 1)
    )
    attn_scale = gains_out(gains, 0, quarter).astype(jnp.float32)
    mlp_scale = gains_out(gains, 1, quarter).astype(jnp.float32)
    inputs = jnp.swapaxes(layer_input, 0, 1).astype(jnp.float32)
    cotangent = jnp.swapaxes(output_cotangent, 0, 1)
    cos_table, sine_table = half_tables(length)
    own_cos = lax.dynamic_slice_in_dim(cos_table, ctx_index * block_len, block_len, 1)
    own_sine = lax.dynamic_slice_in_dim(sine_table, ctx_index * block_len, block_len, 1)
    prefix = lax.dynamic_slice_in_dim(prefix_len, ctx_index * seq_count // places, 1, 0)
    normed_low = norm_rows(inputs, attn_scale).astype(low)
    blocks_shape = (places, features, block_len)

    def project(matrix, rotated):
        product = matmul("bsd,de->bes", normed_low, matrix)
        if rotated:
            heads = product.reshape(seq_count, local // HEAD_DIM, 2, HEAD_DIM // 2, block_len)
            first, second = heads[:, :, 0], heads[:, :, 1]
            product = jnp.stack(
                [first * own_cos - second * own_sine, second * own_cos + first * own_sine], axis=2
            )
        return product.astype(low).reshape(blocks_shape)

    blocks = swap_blocks(
        [project(full_query, True), project(full_key, True), project(full_value, False)], 2
    )
    mixed_heads, log_total = attend(blocks, prefix)
    mixed_low = swap_blocks([mixed_heads], 3).reshape(seq_count, local, block_len)
    hidden = inputs + both_cores(matmul("bes,de->bsd", mixed_low, full_out))
    hnorm_low = norm_rows(hidden, mlp_scale).astype(low)
    gate_out = matmul("bsd,df->bsf", hnorm_low, full_gate)
    up_out = matmul("bsd,df->bsf", hnorm_low, full_up)
    gate_sigmoid = jax.nn.sigmoid(gate_out)
    silu = gate_out * gate_sigmoid
    activated = (silu * up_out).astype(low)
    layer_output = (hidden + both_cores(matmul("bsf,df->bsd", activated, full_down))).astype(low)
    down_w_grad = matmul("bsd,bsf->df", cotangent, activated)
    act_grad = matmul("bsd,df->bsf", cotangent, full_down)
    gate_grad = (
        act_grad * up_out * (gate_sigmoid * (1.0 + gate_out * (1.0 - gate_sigmoid)))
    ).astype(low)
    up_grad = (act_grad * silu).astype(low)
    hnorm_part = matmul("bsf,df->bsd", gate_grad, full_gate) + matmul(
        "bsf,df->bsd", up_grad, full_up
    )
    hnorm_grad = both_cores(hnorm_part)
    gate_w_grad = matmul("bsd,bsf->df", hnorm_low, gate_grad)
    up_w_grad = matmul("bsd,bsf->df", hnorm_low, up_grad)
    hidden_back, mlp_gain_part = norm_back(hidden, mlp_scale, hnorm_grad)
    hidden_grad = cotangent.astype(jnp.float32) + hidden_back
    hidden_low = hidden_grad.astype(low)
    attn_grad = matmul("bsd,de->bes", hidden_low, full_out).astype(low)
    back = swap_blocks([attn_grad.reshape(blocks_shape)], 4)
    out_w_grad = matmul("bsd,bes->de", hidden_low, mixed_low)
    grads = attend_back_heads(blocks, back, log_total, prefix, cos_table, sine_table)
    grads = swap_blocks([grads[0], grads[1], grads[2]], 5)
    grads = grads.reshape(3, seq_count, local, block_len)
    normed_part = (
        matmul("bes,de->bsd", grads[0], full_query)
        + matmul("bes,de->bsd", grads[1], full_key)
        + matmul("bes,de->bsd", grads[2], full_value)
    )
    normed_grad = both_cores(normed_part)
    input_back, attn_gain_part = norm_back(inputs, attn_scale, normed_grad)
    input_grad = (hidden_grad + input_back).astype(low)
    weight_grads = [
        down_w_grad,
        gate_w_grad,
        up_w_grad,
        out_w_grad,
        matmul("bsd,bes->de", normed_low, grads[0]),
        matmul("bsd,bes->de", normed_low, grads[1]),
        matmul("bsd,bes->de", normed_low, grads[2]),
    ]
    count = lax.axis_size("fsdp")
    gain_parts = jax.vmap(gains_in)(
        attn_gain_part.reshape(count, -1), mlp_gain_part.reshape(count, -1)
    ).reshape(-1, 128)
    reduced = reduce_grads([gain_parts] + [grad.astype(low) for grad in weight_grads], 6)
    gains, down, gate, up, out, query, key, value = [
        total.astype(jnp.float32) for total in reduced
    ]
    return (
        jnp.swapaxes(layer_output, 0, 1),
        jnp.swapaxes(input_grad, 0, 1),
        gains_out(gains, 0, quarter),
        gains_out(gains, 1, quarter),
        query,
        key,
        value,
        out.T,
        gate,
        up,
        down.T,
    )


def heads_divide(mesh, args):
    block_rows = args[0].shape[0] // mesh.shape["ctx"]
    seqs = args[0].shape[1] // mesh.shape["fsdp"]
    heads = args[5].shape[1] // mesh.shape["tp"] // HEAD_DIM
    places = mesh.shape["ctx"]
    return (
        places == 4
        and mesh.shape["fsdp"] > 1
        and places % seqs == 0
        and heads % (places // seqs) == 0
        and block_rows % 256 == 0
    )


def solution(mesh):
    placed = (
        P("ctx", "fsdp", None),
        P("ctx", "fsdp", None),
        P("fsdp"),
        P("fsdp"),
        P("fsdp"),
        P("fsdp", "tp"),
        P("fsdp", "tp"),
        P("fsdp", "tp"),
        P("tp", "fsdp"),
        P("fsdp", "tp"),
        P("fsdp", "tp"),
        P("tp", "fsdp"),
    )
    def step(*args):
        chosen = heads_body if heads_divide(mesh, args) else body
        return spread_over(chosen)(*args)

    def spread_over(chosen):
      return jax.shard_map(
        chosen,
        mesh=mesh,
        in_specs=placed,
        out_specs=(
            P("ctx", "fsdp", None),
            P("ctx", "fsdp", None),
            P("fsdp"),
            P("fsdp"),
            P("fsdp", "tp"),
            P("fsdp", "tp"),
            P("fsdp", "tp"),
            P("tp", "fsdp"),
            P("fsdp", "tp"),
            P("fsdp", "tp"),
            P("tp", "fsdp"),
        ),
        check_vma=False,
    )

    return step
```

```python
import functools
import math

import jax
import jax.numpy as jnp
from jax import lax
from jax.experimental import pallas as pl
from jax.experimental.pallas import tpu as pltpu
from jax.sharding import PartitionSpec as P

HEAD_DIM = 64


EPS = 1e-06
BASE = 10000.0
MASKED = -1e30


def partner(block, axis, apart):
    count = lax.axis_size(axis)
    route = []
    for low in range(count):
        high = low | 1 << apart
        if high != low and high < count:
            route += [(low, high), (high, low)]
    return lax.ppermute(block, axis, route)


def from_behind(value, axis, steps):
    count = lax.axis_size(axis)
    pairs = [(source, (source + steps) % count) for source in range(count)]
    return lax.ppermute(value, axis, pairs)


def norm_rows(values, gain):
    return values * lax.rsqrt(jnp.mean(values * values, axis=-1, keepdims=True) + EPS) * gain


def rope_tables(positions):
    half_dim = HEAD_DIM // 2
    frequency = jnp.exp(
        jnp.arange(half_dim, dtype=jnp.float32) * (-2.0 * math.log(BASE) / HEAD_DIM)
    )
    angles = positions.astype(jnp.float32)[:, None] * frequency[None, :]
    cos_table = jnp.concatenate([jnp.cos(angles), jnp.cos(angles)], axis=1)
    sine_table = jnp.concatenate([jnp.sin(angles), jnp.sin(angles)], axis=1)
    return (cos_table[:, None, None, :], sine_table[:, None, None, :])


def rotary(values, cos_table, sine_table):
    half_dim = values.shape[-1] // 2
    turned = jnp.concatenate([-values[..., half_dim:], values[..., :half_dim]], axis=-1)
    return values * cos_table + turned * sine_table


def unrotary(grads, cos_table, sine_table):
    half_dim = grads.shape[-1] // 2
    scaled = grads * sine_table
    turned = jnp.concatenate([scaled[..., half_dim:], -scaled[..., :half_dim]], axis=-1)
    return grads * cos_table + turned


def block_positions(device, block_len, ctx_size):
    half_len = block_len // 2
    steps = jnp.arange(half_len, dtype=jnp.int32)
    first_part = 2 * device * half_len + steps
    second_part = (2 * ctx_size - 1 - 2 * device) * half_len + steps
    return jnp.concatenate([first_part, second_part], axis=0)


def mirror_rows(values):
    ctx_bits = lax.axis_size("ctx").bit_length() - 1
    for bit in range(ctx_bits):
        values = partner(values, "ctx", bit)
    return values


def visible(prefix_len, query_pos, key_pos):
    causal = key_pos[None, :] <= query_pos[:, None]
    opened = key_pos[None, None, :] < prefix_len[:, None, None]
    return (causal[None] | opened)[:, None]


def block_needed(prefix_len, query_pos, key_pos):
    first_key = jnp.min(key_pos)
    return (first_key <= jnp.max(query_pos)) | jnp.any(prefix_len > first_key)


def attend_step(softmax_state, queries, key_value, prefix_len, query_pos, key_pos):
    key_heads = key_value[..., :HEAD_DIM]
    value_heads = key_value[..., HEAD_DIM:]

    def compute(state_in):
        row_max, row_sum, weighted = state_in
        scores = jnp.einsum(
            "qshd,kshd->shqk", queries, key_heads, preferred_element_type=jnp.float32
        ) * HEAD_DIM ** (-0.5)
        allowed = visible(prefix_len, query_pos, key_pos)
        block_max = jnp.max(jnp.where(allowed, scores, MASKED), axis=-1)
        fresh_max = jnp.maximum(row_max, block_max)
        exps = jnp.where(allowed, jnp.exp(scores - fresh_max[..., None]), 0.0)
        factor = jnp.exp(row_max - fresh_max)
        row_sum = row_sum * factor + jnp.sum(exps, axis=-1)
        weighted = weighted * jnp.transpose(factor, (2, 0, 1))[..., None] + jnp.einsum(
            "shqk,kshd->qshd",
            exps.astype(jnp.bfloat16),
            value_heads,
            preferred_element_type=jnp.float32,
        )
        return (fresh_max, row_sum, weighted)

    def skipped(state_in):
        return state_in

    return lax.cond(block_needed(prefix_len, query_pos, key_pos), compute, skipped, softmax_state)


def attend_back(
    queries, attn_grad, log_total, delta_rows, key_value, prefix_len, query_pos, key_pos
):
    key_heads = key_value[..., :HEAD_DIM]
    value_heads = key_value[..., HEAD_DIM:]
    score_scale = HEAD_DIM ** (-0.5)

    def compute(unused):
        scores = (
            jnp.einsum("qshd,kshd->shqk", queries, key_heads, preferred_element_type=jnp.float32)
            * score_scale
        )
        allowed = visible(prefix_len, query_pos, key_pos)
        probabilities = jnp.where(allowed, jnp.exp(scores - log_total[..., None]), 0.0)
        prob_grad = jnp.einsum(
            "qshd,kshd->shqk", attn_grad, value_heads, preferred_element_type=jnp.float32
        )
        score_grad = (probabilities * (prob_grad - delta_rows[..., None])).astype(jnp.bfloat16)
        query_part = (
            jnp.einsum("shqk,kshd->qshd", score_grad, key_heads, preferred_element_type=jnp.float32)
            * score_scale
        )
        key_part = (
            jnp.einsum("shqk,qshd->kshd", score_grad, queries, preferred_element_type=jnp.float32)
            * score_scale
        )
        value_part = jnp.einsum(
            "shqk,qshd->kshd",
            probabilities.astype(jnp.bfloat16),
            attn_grad,
            preferred_element_type=jnp.float32,
        )
        return (query_part, jnp.concatenate([key_part, value_part], axis=-1))

    def skipped(unused):
        return (jnp.zeros(queries.shape, jnp.float32), jnp.zeros(key_value.shape, jnp.float32))

    return lax.cond(block_needed(prefix_len, query_pos, key_pos), compute, skipped, 0)


def pass_grads(key_grads):
    return from_behind(key_grads.astype(jnp.bfloat16), "ctx", 1).astype(key_grads.dtype)


def body(
    layer_input,
    output_cotangent,
    prefix_len,
    attn_gain,
    mlp_gain,
    query_weight,
    key_weight,
    value_weight,
    out_weight,
    gate_weight,
    up_weight,
    down_weight,
):
    block_len, seq_count, width = layer_input.shape
    half_len = block_len // 2
    ctx_size = lax.axis_size("ctx")
    ctx_index = lax.axis_index("ctx")
    moved = mirror_rows(jnp.stack([layer_input[half_len:], output_cotangent[half_len:]], axis=0))
    layer_input = jnp.concatenate([layer_input[:half_len], moved[0]], axis=0)
    output_cotangent = jnp.concatenate([output_cotangent[:half_len], moved[1]], axis=0)
    query_pos = block_positions(ctx_index, block_len, ctx_size)
    cos_table, sine_table = rope_tables(query_pos)
    gain_one, full_query, full_key, full_value, full_out = (
        lax.all_gather(attn_gain.astype(jnp.bfloat16), "fsdp", axis=0, tiled=True),
        lax.all_gather(query_weight.astype(jnp.bfloat16), "fsdp", axis=0, tiled=True),
        lax.all_gather(key_weight.astype(jnp.bfloat16), "fsdp", axis=0, tiled=True),
        lax.all_gather(value_weight.astype(jnp.bfloat16), "fsdp", axis=0, tiled=True),
        lax.all_gather(out_weight.astype(jnp.bfloat16), "fsdp", axis=1, tiled=True),
    )
    gain_two, full_gate, full_up, full_down = (
        lax.all_gather(mlp_gain.astype(jnp.bfloat16), "fsdp", axis=0, tiled=True),
        lax.all_gather(gate_weight.astype(jnp.bfloat16), "fsdp", axis=0, tiled=True),
        lax.all_gather(up_weight.astype(jnp.bfloat16), "fsdp", axis=0, tiled=True),
        lax.all_gather(down_weight.astype(jnp.bfloat16), "fsdp", axis=1, tiled=True),
    )
    heads_local = full_query.shape[1] // HEAD_DIM
    inputs = layer_input.astype(jnp.float32)
    attn_scale = gain_one.astype(jnp.float32)
    normed_low = norm_rows(inputs, attn_scale).astype(jnp.bfloat16)

    def project(matrix):
        product = jnp.einsum("bsd,de->bse", normed_low, matrix, preferred_element_type=jnp.float32)
        return product.reshape(block_len, seq_count, heads_local, HEAD_DIM)

    queries = rotary(project(full_query), cos_table, sine_table).astype(jnp.bfloat16)
    key_heads = rotary(project(full_key), cos_table, sine_table).astype(jnp.bfloat16)
    value_heads = project(full_value).astype(jnp.bfloat16)
    key_value = jnp.concatenate([key_heads, value_heads], axis=-1)
    stats_shape = (seq_count, heads_local, block_len)
    initial = (
        jnp.full(stats_shape, MASKED, jnp.float32),
        jnp.zeros(stats_shape, jnp.float32),
        jnp.zeros((block_len, seq_count, heads_local, HEAD_DIM), jnp.float32),
    )
    softmax_state = attend_step(initial, queries, key_value, prefix_len, query_pos, query_pos)

    def forward_shift(counter, loop_carry):
        state_in, moving = loop_carry
        moving = from_behind(moving, "ctx", 1)
        source = (ctx_index - counter) % ctx_size
        key_pos = block_positions(source, block_len, ctx_size)
        state_in = attend_step(state_in, queries, moving, prefix_len, query_pos, key_pos)
        return (state_in, moving)

    softmax_state, unused_keys = lax.fori_loop(
        1, ctx_size, forward_shift, (softmax_state, key_value)
    )
    row_max, row_sum, weighted = softmax_state
    log_total = row_max + jnp.log(row_sum)
    attn_exact = weighted / jnp.transpose(row_sum, (2, 0, 1))[..., None]
    mixed_low = attn_exact.reshape(block_len, seq_count, heads_local * HEAD_DIM).astype(
        jnp.bfloat16
    )
    attn_part = jnp.einsum("bse,ed->bsd", mixed_low, full_out, preferred_element_type=jnp.float32)
    hidden = inputs + lax.psum(attn_part.astype(jnp.bfloat16), "tp").astype(jnp.float32)
    mlp_scale = gain_two.astype(jnp.float32)
    hnorm_low = norm_rows(hidden, mlp_scale).astype(jnp.bfloat16)
    gate_out = jnp.einsum("bsd,df->bsf", hnorm_low, full_gate, preferred_element_type=jnp.float32)
    up_out = jnp.einsum("bsd,df->bsf", hnorm_low, full_up, preferred_element_type=jnp.float32)
    activated = (jax.nn.silu(gate_out) * up_out).astype(jnp.bfloat16)
    down_part = jnp.einsum("bsf,fd->bsd", activated, full_down, preferred_element_type=jnp.float32)
    result = hidden + lax.psum(down_part.astype(jnp.bfloat16), "tp").astype(jnp.float32)
    layer_output = result.astype(jnp.bfloat16)
    grad_float = output_cotangent.astype(jnp.float32)
    down_w_grad = jnp.einsum(
        "bsf,bsd->fd", activated, output_cotangent, preferred_element_type=jnp.float32
    )
    act_grad = jnp.einsum(
        "bsd,fd->bsf", output_cotangent, full_down, preferred_element_type=jnp.float32
    )
    unused_value, silu_pullback = jax.vjp(
        lambda gate_in, up_in: jax.nn.silu(gate_in) * up_in, gate_out, up_out
    )
    gate_back, up_back = silu_pullback(act_grad)
    gate_grad = gate_back.astype(jnp.bfloat16)
    up_grad = up_back.astype(jnp.bfloat16)
    gate_w_grad = jnp.einsum(
        "bsd,bsf->df", hnorm_low, gate_grad, preferred_element_type=jnp.float32
    )
    up_w_grad = jnp.einsum("bsd,bsf->df", hnorm_low, up_grad, preferred_element_type=jnp.float32)
    hnorm_part = jnp.einsum(
        "bsf,df->bsd", gate_grad, full_gate, preferred_element_type=jnp.float32
    ) + jnp.einsum("bsf,df->bsd", up_grad, full_up, preferred_element_type=jnp.float32)
    hnorm_grad = lax.psum(hnorm_part.astype(jnp.bfloat16), "tp").astype(jnp.float32)
    unused_norm, norm_pullback = jax.vjp(norm_rows, hidden, mlp_scale)
    hidden_back, mlp_gain_part = norm_pullback(hnorm_grad)
    hidden_grad = grad_float + hidden_back
    hidden_low = hidden_grad.astype(jnp.bfloat16)
    out_w_grad = jnp.einsum(
        "bse,bsd->ed", mixed_low, hidden_low, preferred_element_type=jnp.float32
    )
    attn_grad = jnp.einsum(
        "bsd,ed->bse", hidden_low, full_out, preferred_element_type=jnp.float32
    ).astype(jnp.bfloat16)
    attn_grad = attn_grad.reshape(block_len, seq_count, heads_local, HEAD_DIM)
    delta_rows = jnp.transpose(
        jnp.sum(attn_grad.astype(jnp.float32) * attn_exact, axis=-1), (1, 2, 0)
    )
    zero_query = jnp.zeros((block_len, seq_count, heads_local, HEAD_DIM), jnp.float32)

    def backward_shift(counter, loop_carry):
        query_acc, moving, travelling = loop_carry
        source = (ctx_index - counter) % ctx_size
        key_pos = block_positions(source, block_len, ctx_size)
        query_part, key_part = attend_back(
            queries, attn_grad, log_total, delta_rows, moving, prefix_len, query_pos, key_pos
        )
        travelling = pass_grads(travelling + key_part)
        moving = from_behind(moving, "ctx", 1)
        return (query_acc + query_part, moving, travelling)

    travel_zero = jnp.zeros((block_len, seq_count, heads_local, 2 * HEAD_DIM), jnp.float32)
    query_acc, moving, travelling = lax.fori_loop(
        0, ctx_size - 1, backward_shift, (zero_query, key_value, travel_zero)
    )
    last_source = (ctx_index + 1) % ctx_size
    last_pos = block_positions(last_source, block_len, ctx_size)
    query_part, key_part = attend_back(
        queries, attn_grad, log_total, delta_rows, moving, prefix_len, query_pos, last_pos
    )
    query_acc = query_acc + query_part
    own_grads = pass_grads(travelling + key_part)
    flat_shape = (block_len, seq_count, heads_local * HEAD_DIM)
    query_grad = unrotary(query_acc, cos_table, sine_table).astype(jnp.bfloat16).reshape(flat_shape)
    key_grad = (
        unrotary(own_grads[..., :HEAD_DIM], cos_table, sine_table)
        .astype(jnp.bfloat16)
        .reshape(flat_shape)
    )
    value_grad = own_grads[..., HEAD_DIM:].astype(jnp.bfloat16).reshape(flat_shape)
    query_w_grad = jnp.einsum(
        "bsd,bse->de", normed_low, query_grad, preferred_element_type=jnp.float32
    )
    key_w_grad = jnp.einsum("bsd,bse->de", normed_low, key_grad, preferred_element_type=jnp.float32)
    value_w_grad = jnp.einsum(
        "bsd,bse->de", normed_low, value_grad, preferred_element_type=jnp.float32
    )
    normed_part = (
        jnp.einsum("bse,de->bsd", query_grad, full_query, preferred_element_type=jnp.float32)
        + jnp.einsum("bse,de->bsd", key_grad, full_key, preferred_element_type=jnp.float32)
        + jnp.einsum("bse,de->bsd", value_grad, full_value, preferred_element_type=jnp.float32)
    )
    normed_grad = lax.psum(normed_part.astype(jnp.bfloat16), "tp").astype(jnp.float32)
    unused_first, first_pullback = jax.vjp(norm_rows, inputs, attn_scale)
    input_back, attn_gain_part = first_pullback(normed_grad)
    input_grad = (hidden_grad + input_back).astype(jnp.bfloat16)
    returned = mirror_rows(jnp.stack([layer_output[half_len:], input_grad[half_len:]], axis=0))
    layer_output = jnp.concatenate([layer_output[:half_len], returned[0]], axis=0)
    input_grad = jnp.concatenate([input_grad[:half_len], returned[1]], axis=0)
    shards = (
        lax.psum_scatter(
            attn_gain_part.astype(jnp.bfloat16), "fsdp", scatter_dimension=0, tiled=True
        ).astype(jnp.float32),
        lax.psum_scatter(
            mlp_gain_part.astype(jnp.bfloat16), "fsdp", scatter_dimension=0, tiled=True
        ).astype(jnp.float32),
        lax.psum_scatter(
            query_w_grad.astype(jnp.bfloat16), "fsdp", scatter_dimension=0, tiled=True
        ).astype(jnp.float32),
        lax.psum_scatter(
            key_w_grad.astype(jnp.bfloat16), "fsdp", scatter_dimension=0, tiled=True
        ).astype(jnp.float32),
        lax.psum_scatter(
            value_w_grad.astype(jnp.bfloat16), "fsdp", scatter_dimension=0, tiled=True
        ).astype(jnp.float32),
        lax.psum_scatter(
            out_w_grad.astype(jnp.bfloat16), "fsdp", scatter_dimension=1, tiled=True
        ).astype(jnp.float32),
        lax.psum_scatter(
            gate_w_grad.astype(jnp.bfloat16), "fsdp", scatter_dimension=0, tiled=True
        ).astype(jnp.float32),
        lax.psum_scatter(
            up_w_grad.astype(jnp.bfloat16), "fsdp", scatter_dimension=0, tiled=True
        ).astype(jnp.float32),
        lax.psum_scatter(
            down_w_grad.astype(jnp.bfloat16), "fsdp", scatter_dimension=1, tiled=True
        ).astype(jnp.float32),
    )
    totals = (
        lax.psum(shards[0].astype(jnp.bfloat16), "ctx").astype(jnp.float32),
        lax.psum(shards[1].astype(jnp.bfloat16), "ctx").astype(jnp.float32),
        lax.psum(shards[2].astype(jnp.bfloat16), "ctx").astype(jnp.float32),
        lax.psum(shards[3].astype(jnp.bfloat16), "ctx").astype(jnp.float32),
        lax.psum(shards[4].astype(jnp.bfloat16), "ctx").astype(jnp.float32),
        lax.psum(shards[5].astype(jnp.bfloat16), "ctx").astype(jnp.float32),
        lax.psum(shards[6].astype(jnp.bfloat16), "ctx").astype(jnp.float32),
        lax.psum(shards[7].astype(jnp.bfloat16), "ctx").astype(jnp.float32),
        lax.psum(shards[8].astype(jnp.bfloat16), "ctx").astype(jnp.float32),
    )
    return (
        layer_output,
        input_grad,
        totals[0],
        totals[1],
        totals[2],
        totals[3],
        totals[4],
        totals[5],
        totals[6],
        totals[7],
        totals[8],
    )


MESH = pl.DeviceIdType.MESH
VMEM_LIMIT = 60 << 20
LINE = 2


def place():
    ctx = lax.axis_index("ctx")
    along_x = ctx + 1 - 2 * lax.rem(ctx, 2)
    along_y = lax.rem(ctx + 2, 4)
    return lax.axis_index("fsdp"), ctx, along_x, along_y, 3 - ctx


def greet(devices):
    barrier = pltpu.get_barrier_semaphore()
    for device in devices:
        pl.semaphore_signal(barrier, inc=1, device_id=device, device_id_type=MESH)
    pl.semaphore_wait(barrier, len(devices))


def rows_at(block, rows):
    return pl.ds(pl.multiple_of(block * rows, 16), rows)


def send(source, target, send_sem, recv_sem, device):
    return pltpu.make_async_remote_copy(
        src_ref=source,
        dst_ref=target,
        send_sem=send_sem,
        recv_sem=recv_sem,
        device_id=device,
        device_id_type=MESH,
    )


def column_chunks(shapes, widest, paths=2):
    chunks = []
    for index, (rows, columns) in enumerate(shapes):
        count = -(-columns // widest)
        while columns % count or (columns // count) % 128:
            count += 1
        width = columns // count
        chunks += [(index, rows // 4, part * width, width) for part in range(count)]
    return [chunk + (number % paths,) for number, chunk in enumerate(chunks)]


def gather_steps(chunks, shard_refs, full_refs, local_sem, send_sems, recv_sems):
    fsdp, ctx, along_x, along_y, across = place()
    last = lax.axis_size("fsdp") - 1

    def region(chunk, shard, quarter):
        index, rows, low, width, path = chunk
        if path == LINE:
            return full_refs[index].at[rows_at(shard, 4 * rows), pl.ds(low, width)]
        return full_refs[index].at[rows_at(shard * 4 + quarter, rows), pl.ds(low, width)]

    def pass_on(number, shard, quarter, kind, device, source=None):
        target = region(chunks[number], shard, quarter)
        return send(
            target if source is None else source,
            target,
            send_sems.at[number, shard, kind],
            recv_sems.at[number, shard, quarter],
            device,
        )

    def own_source(number):
        index, rows, low, width, path = chunks[number]
        if path == LINE:
            return shard_refs[index].at[:, pl.ds(low, width)]
        return shard_refs[index].at[rows_at(ctx, rows), pl.ds(low, width)]

    def arrived(number, shard, quarter):
        pass_on(number, shard, quarter, 0, {"ctx": along_x}).wait_recv()

    count = range(len(chunks))
    up, down = {"fsdp": lax.rem(fsdp + 1, last + 1)}, {"fsdp": lax.rem(fsdp + last, last + 1)}
    to_x, to_y = {"ctx": along_x}, {"ctx": along_y}

    def begin():
        for number in count:

            @pl.when(fsdp < last)
            def _(number=number):
                pass_on(number, fsdp, ctx, 0, up, own_source(number)).start()

            @pl.when(fsdp > 0)
            def _(number=number):
                pass_on(number, fsdp, ctx, 1, down, own_source(number)).start()

        for index, shard_ref in enumerate(shard_refs):
            rows = shard_ref.shape[0]
            pltpu.make_async_copy(
                shard_ref, full_refs[index].at[rows_at(fsdp, rows)], local_sem.at[index]
            ).start()

    def each(steps, act):
        for sign in (-1, 1):
            shard = fsdp + sign * steps

            @pl.when((shard >= 0) & (shard <= last))
            def _(sign=sign, shard=shard):
                act(shard, sign)

    def from_line(number, steps):
        def act(shard, sign):
            arrived(number, shard, ctx)
            if sign < 0:

                @pl.when(fsdp < last)
                def _():
                    pass_on(number, shard, ctx, 0, up).start()

            else:

                @pl.when(fsdp > 0)
                def _():
                    pass_on(number, shard, ctx, 1, down).start()

            if chunks[number][-1] != LINE:
                pass_on(number, shard, ctx, 2, to_x).start()
                pass_on(number, shard, ctx, 3, to_y).start()

        each(steps, act)

    def to_corner(number, steps):
        if chunks[number][-1] == LINE:
            return

        def act(shard, sign):
            if chunks[number][-1] == 0:
                arrived(number, shard, along_x)
                pass_on(number, shard, along_x, 4, to_y).start()
            else:
                arrived(number, shard, along_y)
                pass_on(number, shard, along_y, 4, to_x).start()

        each(steps, act)

    def finish():
        for steps in range(1, last + 1):
            for number in count:

                def act(shard, sign, number=number):
                    if chunks[number][-1] != LINE:
                        arrived(number, shard, along_y if chunks[number][-1] == 0 else along_x)
                        arrived(number, shard, across)
                    forward = fsdp < last if sign < 0 else fsdp > 0

                    @pl.when(forward)
                    def _():
                        pass_on(number, shard, ctx, 0 if sign < 0 else 1, up).wait_send()

                    if chunks[number][-1] != LINE:
                        for kind in (2, 3, 4):
                            pass_on(number, shard, ctx, kind, to_x).wait_send()

                each(steps, act)
        for number in count:

            @pl.when(fsdp < last)
            def _(number=number):
                pass_on(number, fsdp, ctx, 0, up, own_source(number)).wait_send()

            @pl.when(fsdp > 0)
            def _(number=number):
                pass_on(number, fsdp, ctx, 1, down, own_source(number)).wait_send()

        for index, shard_ref in enumerate(shard_refs):
            rows = shard_ref.shape[0]
            pltpu.make_async_copy(
                shard_ref, full_refs[index].at[rows_at(fsdp, rows)], local_sem.at[index]
            ).wait()

    return begin, from_line, to_corner, finish


def neighbours(fsdp, along_x, along_y):
    size = lax.axis_size("fsdp")
    return [
        {"ctx": along_x},
        {"ctx": along_y},
        {"fsdp": lax.rem(fsdp + 1, size)},
        {"fsdp": lax.rem(fsdp + size - 1, size)},
    ]


def gather_kernel(chunks, arrays, *refs):
    shard_refs, full_refs = refs[:arrays], refs[arrays : 2 * arrays]
    local_sem, send_sems, recv_sems = refs[2 * arrays :]
    fsdp, ctx, along_x, along_y, across = place()
    greet(neighbours(fsdp, along_x, along_y))
    begin, from_line, to_corner, finish = gather_steps(
        chunks, shard_refs, full_refs, local_sem, send_sems, recv_sems
    )
    begin()
    last = lax.axis_size("fsdp") - 1
    for steps in range(1, last + 2):
        for number in range(len(chunks)):
            if steps <= last:
                from_line(number, steps)
            if steps > 1:
                to_corner(number, steps - 1)
    finish()


def gather_scratch(shards, chunks):
    return [
        pltpu.SemaphoreType.DMA((len(shards),)),
        pltpu.SemaphoreType.DMA((len(chunks), 4, 5)),
        pltpu.SemaphoreType.DMA((len(chunks), 4, 4)),
    ]


def gather_shards(shards, collective_id):
    chunks = column_chunks([shard.shape for shard in shards], 512)
    size = lax.axis_size("fsdp")
    anywhere = pl.BlockSpec(memory_space=pl.ANY)
    return pl.pallas_call(
        functools.partial(gather_kernel, chunks, len(shards)),
        out_shape=[
            jax.ShapeDtypeStruct((size * shard.shape[0], shard.shape[1]), shard.dtype)
            for shard in shards
        ],
        in_specs=[pl.BlockSpec(memory_space=pltpu.VMEM)] * len(shards),
        out_specs=[anywhere] * len(shards),
        scratch_shapes=gather_scratch(shards, chunks),
        compiler_params=pltpu.CompilerParams(
            collective_id=collective_id, has_side_effects=True, vmem_limit_bytes=VMEM_LIMIT
        ),
        name="gather_shards",
    )(*shards)


def reduce_steps(chunks, full_refs, out_refs, rest):
    count = len(chunks)
    buffers = [rest[6 * number : 6 * number + 6] for number in range(count)]
    load_sems, send_sems, recv_sems = rest[6 * count :]
    fsdp, ctx, along_x, along_y, across = place()
    size = lax.axis_size("fsdp")
    others = [{"fsdp": lax.rem(fsdp + step, size)} for step in range(1, size)]

    def quarter_of(number, quarter):
        index, rows, low, width, _ = chunks[number]
        return full_refs[index].at[:, rows_at(quarter, rows), pl.ds(low, width)]

    def result(number, quarter):
        index, rows, low, width, _ = chunks[number]
        return out_refs[index].at[rows_at(quarter, rows), pl.ds(low, width)]

    def first_second(number):
        return (along_x, along_y) if chunks[number][-1] == 0 else (along_y, along_x)

    def exchange(number, part):
        first, _ = first_second(number)
        return send(
            quarter_of(number, first if part == 0 else across),
            buffers[number][1].at[part],
            send_sems.at[number, part],
            recv_sems.at[number, part],
            {"ctx": first},
        )

    def load(number, part):
        _, second = first_second(number)
        return pltpu.make_async_copy(
            quarter_of(number, ctx if part == 0 else second),
            buffers[number][0].at[part],
            load_sems.at[number, part],
        )

    def second_hop(number):
        _, second = first_second(number)
        return send(
            buffers[number][2],
            buffers[number][3],
            send_sems.at[number, 2],
            recv_sems.at[number, 2],
            {"ctx": second},
        )

    def along_line(number, step):
        return send(
            buffers[number][4].at[lax.rem(fsdp + step, size)],
            buffers[number][5].at[step - 1],
            send_sems.at[number, 2 + step],
            recv_sems.at[number, 2 + step],
            others[step - 1],
        )

    def spread(number, quarter, kind, target):
        place_there = result(number, quarter)
        return send(
            place_there,
            place_there,
            send_sems.at[number, 2 + size + kind],
            recv_sems.at[number, 2 + size + kind],
            {"ctx": target},
        )

    def stage(number, at):
        first, second = first_second(number)
        own, landed, passing, arrived, total, line = buffers[number]
        if at == 0:
            for part in (1, 0):
                exchange(number, part).start()
                load(number, part).start()
        elif at == 1:
            load(number, 1).wait()
            exchange(number, 1).wait_recv()
            passing[...] = (own[1].astype(jnp.float32) + landed[1].astype(jnp.float32)).astype(
                jnp.bfloat16
            )
            second_hop(number).start()
        elif at == 2:
            load(number, 0).wait()
            exchange(number, 0).wait_recv()
            second_hop(number).wait_recv()
            total[...] = (
                own[0].astype(jnp.float32)
                + landed[0].astype(jnp.float32)
                + arrived[...].astype(jnp.float32)
            ).astype(jnp.bfloat16)
            for step in range(1, size):
                along_line(number, step).start()
        elif at == 3:
            value = total[fsdp].astype(jnp.float32)
            for step in range(1, size):
                along_line(number, step).wait_recv()
                value = value + line[step - 1].astype(jnp.float32)
            index, rows, low, width, _ = chunks[number]
            out_refs[index][rows_at(ctx, rows), pl.ds(low, width)] = value.astype(jnp.bfloat16)
            spread(number, ctx, 0, first).start()
            spread(number, ctx, 1, second).start()
        elif at == 4:
            spread(number, first, 0, first).wait_recv()
            spread(number, first, 2, second).start()
        else:
            spread(number, second, 1, second).wait_recv()
            spread(number, across, 2, second).wait_recv()
            for part in (0, 1):
                exchange(number, part).wait_send()
            second_hop(number).wait_send()
            for step in range(1, size):
                along_line(number, step).wait_send()
            for kind in range(3):
                spread(number, ctx, kind, first).wait_send()

    return stage


def reduce_order(count, lag):
    return [
        (number, at)
        for tick in range(count + 4 * lag)
        for at in range(5, 0, -1)
        for number in (tick - (at - 1) * lag,)
        if 0 <= number < count
    ]


def close_by():
    fsdp, ctx, along_x, along_y, across = place()
    size = lax.axis_size("fsdp")
    return [{"ctx": along_x}, {"ctx": along_y}, {"ctx": across}] + [
        {"fsdp": lax.rem(fsdp + step, size)} for step in range(1, size)
    ]


def reduce_kernel(chunks, arrays, *refs):
    greet(close_by())
    stage = reduce_steps(chunks, refs[:arrays], refs[arrays : 2 * arrays], refs[2 * arrays :])
    for number in range(len(chunks)):
        stage(number, 0)
    for number, at in reduce_order(len(chunks), 2):
        stage(number, at)


def reduce_scratch(chunks, size):
    scratch = []
    for _, rows, _, width, _ in chunks:
        block = (size, rows, width)
        for shape in ((2,) + block, (2,) + block, block, block, block, (size - 1, rows, width)):
            scratch.append(pltpu.VMEM(shape, jnp.bfloat16))
    return scratch + [
        pltpu.SemaphoreType.DMA((len(chunks), 2)),
        pltpu.SemaphoreType.DMA((len(chunks), size + 5)),
        pltpu.SemaphoreType.DMA((len(chunks), size + 5)),
    ]


def reduce_grads(grads, collective_id):
    size = lax.axis_size("fsdp")
    shapes = [(grad.shape[0] // size, grad.shape[1]) for grad in grads]
    chunks = column_chunks(shapes, 512)
    anywhere = pl.BlockSpec(memory_space=pl.ANY)
    return pl.pallas_call(
        functools.partial(reduce_kernel, chunks, len(grads)),
        out_shape=[jax.ShapeDtypeStruct(shape, jnp.bfloat16) for shape in shapes],
        in_specs=[anywhere] * len(grads),
        out_specs=[pl.BlockSpec(memory_space=pltpu.VMEM)] * len(grads),
        scratch_shapes=reduce_scratch(chunks, size),
        compiler_params=pltpu.CompilerParams(
            collective_id=collective_id, has_side_effects=True, vmem_limit_bytes=VMEM_LIMIT
        ),
        name="reduce_grads",
    )(*[grad.reshape(size, shape[0], shape[1]) for grad, shape in zip(grads, shapes)])


def head_rows(head):
    return pl.ds(pl.multiple_of(head * HEAD_DIM, HEAD_DIM), HEAD_DIM)


def swap_steps(sources, landings, local_sems, send_sems, recv_sems):
    fsdp, ctx, along_x, along_y, across = place()
    targets = (across, along_x, along_y)

    def copies(head, local=True):
        rows = head_rows(head)
        made = []
        for index, (source, landing) in enumerate(zip(sources, landings)):
            for number, target in enumerate(targets):
                made.append(
                    send(
                        source.at[target, rows],
                        landing.at[ctx, rows],
                        send_sems.at[head, index, number],
                        recv_sems.at[head, index, number],
                        {"ctx": target},
                    )
                )
            if local:
                made.append(
                    pltpu.make_async_copy(
                        source.at[ctx, rows], landing.at[ctx, rows], local_sems.at[head, index]
                    )
                )
        return made

    def begin(head):
        for copy in copies(head):
            copy.start()

    def landed(head):
        for number, copy in enumerate(copies(head)):
            if number % 4 == 3:
                copy.wait()
            else:
                copy.wait_recv()

    def sent(head):
        for copy in copies(head, local=False):
            copy.wait_send()

    return begin, landed, sent


def swap_scratch(heads, arrays):
    return [
        pltpu.SemaphoreType.DMA((heads, arrays)),
        pltpu.SemaphoreType.DMA((heads, arrays, 3)),
        pltpu.SemaphoreType.DMA((heads, arrays, 3)),
    ]


def beside(head, slot, events):
    for at in sorted({event[0] for event in events if event[1] == slot}):

        @pl.when(head == at)
        def _(at=at):
            for planned, place_in, act in events:
                if planned == at and place_in == slot:
                    act()


def spaced(acts, slots, heads, first, gap):
    planned, left = [], []
    for number, act in enumerate(acts):
        at = first + int(number * gap)
        if at < slots * heads:
            planned.append((at // slots, at % slots, act))
        else:
            left.append(act)
    return planned, left


def dot(left, right):
    return jnp.dot(left, right, preferred_element_type=jnp.float32)


def turn(block):
    return block.astype(jnp.float32).T.astype(block.dtype)


def seen(prefix, row_block, key_block, rows, keys, values, fill):
    if (key_block + 1) * keys <= row_block * rows + 1:
        return values
    key_pos = key_block * keys + lax.broadcasted_iota(jnp.int32, values.shape, 1)
    row_pos = row_block * rows + lax.broadcasted_iota(jnp.int32, values.shape, 0)
    allowed = key_pos < jnp.maximum(row_pos + 1, prefix)
    return jnp.where(allowed, values, fill)


def key_blocks(row_block, rows, keys, length):
    farthest = max((row_block + 1) * rows, length // 2)
    return range(-(-farthest // keys))


def attend_kernel(rows, chunks, arrays, *refs):
    prefix_ref, query_in, key_in, value_in = refs[:4]
    shard_refs, refs = refs[4 : 4 + arrays], refs[4 + arrays :]
    query_blocks, key_blocks_ref, value_blocks, mixed_out, log_ref = refs[:5]
    full_refs, refs = refs[5 : 5 + arrays], refs[5 + arrays :]
    mixed_ref, query_ref, value_ref = refs[:3]
    fsdp, ctx, along_x, along_y, across = place()
    places, features, keys = query_in.shape
    heads = features // HEAD_DIM
    length = places * keys
    greet(close_by())
    begin, landed, sent = swap_steps(
        (query_in, key_in, value_in), (query_blocks, key_blocks_ref, value_blocks), *refs[3:6]
    )
    begin_back, landed_back, sent_back = swap_steps((mixed_ref,), (mixed_out,), *refs[6:9])
    begin_gather, from_line, to_corner, finish = gather_steps(
        chunks, shard_refs, full_refs, *refs[9:12]
    )
    for head in range(heads):
        begin(head)
    begin_gather()
    last = lax.axis_size("fsdp") - 1
    acts = []
    for steps in range(1, last + 2):
        for number in range(len(chunks)):
            if steps <= last:
                acts.append(functools.partial(from_line, number, steps))
            if steps > 1:
                acts.append(functools.partial(to_corner, number, steps - 1))
    slots = length // rows
    planned, left = spaced(acts, slots, heads, 1, slots * heads / len(acts))
    prefix = prefix_ref[0]

    @pl.loop(0, heads)
    def _(head):
        landed(head)
        inside_rows = head_rows(head)
        for block in range(places):
            span = pl.ds(block * keys, keys)
            query_ref[span, :] = turn(
                query_blocks[block, inside_rows] * jnp.bfloat16(HEAD_DIM ** (-0.5))
            )
            value_ref[span, :] = turn(value_blocks[block, inside_rows])
        for row_block in range(length // rows):
            span = pl.ds(row_block * rows, rows)
            queries = query_ref[span, :]
            scores = []
            for block in key_blocks(row_block, rows, keys, length):
                part = dot(queries, key_blocks_ref[block, inside_rows])
                scores.append(seen(prefix, row_block, block, rows, keys, part, MASKED))
            row_max = functools.reduce(
                jnp.maximum, [jnp.max(part, axis=1, keepdims=True) for part in scores]
            )
            row_sum = jnp.zeros_like(row_max)
            mixed = jnp.zeros((rows, HEAD_DIM), jnp.float32)
            for block, part in enumerate(scores):
                exps = jnp.exp(part - row_max)
                row_sum = row_sum + jnp.sum(exps, axis=1, keepdims=True)
                mixed = mixed + dot(
                    exps.astype(jnp.bfloat16), value_ref[pl.ds(block * keys, keys), :]
                )
            log_ref[head, span, :] = row_max + jnp.log(row_sum)
            block, inside = divmod(row_block * rows, keys)
            mixed_ref[block, inside_rows, pl.ds(inside, rows)] = (mixed / row_sum).T.astype(
                jnp.bfloat16
            )
            beside(head, row_block, planned)
        begin_back(head)

    for act in left:
        act()
    finish()
    for head in range(heads):
        landed_back(head)
        sent(head)
        sent_back(head)


def attend(query, key, value, shards, prefix, collective_id):
    places, features, keys = query.shape
    heads = features // HEAD_DIM
    length = places * keys
    size = lax.axis_size("fsdp")
    chunks = column_chunks([shard.shape for shard in shards], 512)
    chunks = [
        chunk[:-1] + (LINE if number % 2 else number // 2 % 2,)
        for number, chunk in enumerate(chunks)
    ]
    held = pl.BlockSpec(memory_space=pltpu.VMEM)
    anywhere = pl.BlockSpec(memory_space=pl.ANY)
    return pl.pallas_call(
        functools.partial(attend_kernel, min(256, keys), chunks, len(shards)),
        out_shape=[jax.ShapeDtypeStruct(query.shape, jnp.bfloat16)] * 4
        + [jax.ShapeDtypeStruct((heads, length, 1), jnp.float32)]
        + [
            jax.ShapeDtypeStruct((size * shard.shape[0], shard.shape[1]), shard.dtype)
            for shard in shards
        ],
        in_specs=[pl.BlockSpec(memory_space=pltpu.SMEM)] + [held] * (3 + len(shards)),
        out_specs=[held] * 3 + [anywhere, held] + [anywhere] * len(shards),
        scratch_shapes=[
            pltpu.VMEM(query.shape, jnp.bfloat16),
            pltpu.VMEM((length, HEAD_DIM), jnp.bfloat16),
            pltpu.VMEM((length, HEAD_DIM), jnp.bfloat16),
        ]
        + swap_scratch(heads, 3)
        + swap_scratch(heads, 1)
        + gather_scratch(shards, chunks),
        compiler_params=pltpu.CompilerParams(
            collective_id=collective_id, has_side_effects=True, vmem_limit_bytes=VMEM_LIMIT
        ),
        name="attend",
    )(prefix, query, key, value, *shards)


def turn_back(grads, cos_table, sine_table):
    half = HEAD_DIM // 2
    low, high = grads[:half], grads[half:]
    return (
        low * cos_table + high * sine_table,
        high * cos_table - low * sine_table,
    )


def attend_back_kernel(rows, chunks, arrays, *refs):
    prefix_ref, back_in, query_blocks, key_blocks_ref, value_blocks = refs[:5]
    log_ref, cos_ref, sine_ref = refs[5:8]
    weight_refs, refs = refs[8 : 8 + arrays], refs[8 + arrays :]
    landings, reduced_refs, refs = refs[:3], refs[3 : 3 + arrays], refs[3 + arrays :]
    back_ref, query_out, key_out, value_out = refs[:4]
    query_ref, key_ref, attn_ref, key_grad_ref, value_grad_ref = refs[4:9]
    places, features, keys = back_in.shape
    heads = features // HEAD_DIM
    length = places * keys
    half = HEAD_DIM // 2
    scale = HEAD_DIM ** (-0.5)
    greet(close_by())
    begin, landed, sent = swap_steps((back_in,), (back_ref,), *refs[9:12])
    begin_home, landed_home, sent_home = swap_steps(
        (query_out, key_out, value_out), landings, *refs[12:15]
    )
    stage = reduce_steps(chunks, weight_refs, reduced_refs, refs[15:])
    for head in range(heads):
        begin(head)
    for number in range(len(chunks)):
        stage(number, 0)
    acts = [functools.partial(stage, *step) for step in reduce_order(len(chunks), 2)]
    slots = length // rows
    planned, left = spaced(acts, slots, heads, 3, 1.2)
    prefix = prefix_ref[0]

    @pl.loop(0, heads)
    def _(head):
        landed(head)
        inside_rows = head_rows(head)
        for block in range(places):
            span = pl.ds(block * keys, keys)
            query_ref[span, :] = turn(query_blocks[block, inside_rows] * jnp.bfloat16(scale))
            key_ref[span, :] = turn(key_blocks_ref[block, inside_rows])
            attn_ref[span, :] = turn(back_ref[block, inside_rows])
        key_grad_ref[...] = jnp.zeros_like(key_grad_ref)
        value_grad_ref[...] = jnp.zeros_like(value_grad_ref)
        low_rows = pl.ds(pl.multiple_of(head * HEAD_DIM, half), half)
        high_rows = pl.ds(pl.multiple_of(head * HEAD_DIM + half, half), half)
        for row_block in range(length // rows):
            span = pl.ds(row_block * rows, rows)
            home, inside = divmod(row_block * rows, keys)
            lanes = pl.ds(inside, rows)
            queries, attn_grad = query_ref[span, :], attn_ref[span, :]
            queries_low = query_blocks[home, inside_rows, lanes] * jnp.bfloat16(scale)
            attn_low = back_ref[home, inside_rows, lanes]
            total = log_ref[head, span, :]
            reach = key_blocks(row_block, rows, keys, length)
            weights, pulls = [], []
            delta = jnp.zeros((rows, 1), jnp.float32)
            for block in reach:
                part = dot(queries, key_blocks_ref[block, inside_rows])
                part = jnp.exp(seen(prefix, row_block, block, rows, keys, part, MASKED) - total)
                pull = dot(attn_grad, value_blocks[block, inside_rows])
                delta = delta + jnp.sum(part * pull, axis=1, keepdims=True)
                weights.append(part)
                pulls.append(pull)
            query_grad = jnp.zeros((rows, HEAD_DIM), jnp.float32)
            for block in reach:
                key_span = pl.ds(block * keys, keys)
                score_grad = (weights[block] * (pulls[block] - delta)).astype(jnp.bfloat16)
                query_grad = query_grad + dot(score_grad, key_ref[key_span, :])
                key_grad_ref[:, key_span] += dot(queries_low, score_grad)
                value_grad_ref[:, key_span] += dot(attn_low, weights[block].astype(jnp.bfloat16))
            low, high = turn_back((query_grad * scale).T, cos_ref[:, span], sine_ref[:, span])
            query_out[home, low_rows, lanes] = low.astype(jnp.bfloat16)
            query_out[home, high_rows, lanes] = high.astype(jnp.bfloat16)
            beside(head, row_block, planned)
        for block in range(places):
            span = pl.ds(block * keys, keys)
            low, high = turn_back(key_grad_ref[:, span], cos_ref[:, span], sine_ref[:, span])
            key_out[block, low_rows] = low.astype(jnp.bfloat16)
            key_out[block, high_rows] = high.astype(jnp.bfloat16)
            value_out[block, inside_rows] = value_grad_ref[:, span].astype(jnp.bfloat16)
        begin_home(head)

    for act in left:
        act()
    for head in range(heads):
        landed_home(head)
        sent(head)
        sent_home(head)


def attend_back_heads(
    back, blocks, log_total, prefix, cos_table, sine_table, weight_grads, collective_id
):
    places, features, keys = back.shape
    heads = features // HEAD_DIM
    length = places * keys
    size = lax.axis_size("fsdp")
    shapes = [(grad.shape[0] // size, grad.shape[1]) for grad in weight_grads]
    chunks = column_chunks(shapes, 512)
    held = pl.BlockSpec(memory_space=pltpu.VMEM)
    anywhere = pl.BlockSpec(memory_space=pl.ANY)
    return pl.pallas_call(
        functools.partial(attend_back_kernel, min(256, keys), chunks, len(weight_grads)),
        out_shape=[jax.ShapeDtypeStruct(back.shape, jnp.bfloat16)] * 3
        + [jax.ShapeDtypeStruct(shape, jnp.bfloat16) for shape in shapes],
        in_specs=[pl.BlockSpec(memory_space=pltpu.SMEM)]
        + [held] * 7
        + [anywhere] * len(weight_grads),
        out_specs=[anywhere] * 3 + [held] * len(weight_grads),
        scratch_shapes=[pltpu.VMEM(back.shape, jnp.bfloat16)] * 4
        + [pltpu.VMEM((length, HEAD_DIM), jnp.bfloat16)] * 3
        + [pltpu.VMEM((HEAD_DIM, length), jnp.float32)] * 2
        + swap_scratch(heads, 1)
        + swap_scratch(heads, 3)
        + reduce_scratch(chunks, size),
        compiler_params=pltpu.CompilerParams(
            collective_id=collective_id, has_side_effects=True, vmem_limit_bytes=VMEM_LIMIT
        ),
        name="attend_back",
    )(
        prefix,
        back,
        *blocks,
        log_total,
        cos_table,
        sine_table,
        *[grad.reshape(size, shape[0], shape[1]) for grad, shape in zip(weight_grads, shapes)],
    )


def both_cores(part):
    part = part.astype(jnp.bfloat16)
    size = lax.axis_size("tp")
    other = lax.ppermute(part, "tp", [(core, (core + 1) % size) for core in range(size)])
    return part.astype(jnp.float32) + other.astype(jnp.float32)


def matmul(spec, left, right):
    return jnp.einsum(spec, left, right, preferred_element_type=jnp.float32)


def half_tables(length):
    half = HEAD_DIM // 2
    frequency = jnp.exp(jnp.arange(half, dtype=jnp.float32) * (-2.0 * math.log(BASE) / HEAD_DIM))
    angles = frequency[:, None] * jnp.arange(length, dtype=jnp.float32)[None, :]
    return jnp.cos(angles), jnp.sin(angles)


def norm_back(values, gain, grads):
    scale = lax.rsqrt(jnp.mean(values * values, axis=-1, keepdims=True) + EPS)
    pulled = grads * gain
    inner = jnp.mean(values * pulled, axis=-1, keepdims=True)
    gain_part = jnp.sum(grads * values * scale, axis=(0, 1))
    return scale * pulled - values * (scale * scale * scale * inner), gain_part


def gains_in(first, second):
    both = jnp.stack([first.reshape(4, -1), second.reshape(4, -1)], axis=1)
    both = jnp.pad(both, ((0, 0), (0, 14), (0, 128 - both.shape[2])))
    return both.reshape(64, 128).astype(jnp.bfloat16)


def gains_out(packed, which, quarter):
    return packed.reshape(-1, 16, 128)[:, which, :quarter].reshape(-1)


def heads_body(
    layer_input,
    output_cotangent,
    prefix_len,
    attn_gain,
    mlp_gain,
    query_weight,
    key_weight,
    value_weight,
    out_weight,
    gate_weight,
    up_weight,
    down_weight,
):
    block_len, seq_count, width = layer_input.shape
    places = lax.axis_size("ctx")
    ctx_index = lax.axis_index("ctx")
    local = query_weight.shape[1]
    features = seq_count * local // places
    length = places * block_len
    quarter = attn_gain.shape[0] // 4
    low = jnp.bfloat16
    shards = [
        gains_in(attn_gain, mlp_gain),
        query_weight.astype(low),
        key_weight.astype(low),
        value_weight.astype(low),
        out_weight.T.astype(low),
        gate_weight.astype(low),
        up_weight.astype(low),
        down_weight.T.astype(low),
    ]
    gains, full_query, full_key, full_value, full_out = gather_shards(shards[:5], 1)
    attn_scale = gains_out(gains, 0, quarter).astype(jnp.float32)
    mlp_scale = gains_out(gains, 1, quarter).astype(jnp.float32)
    inputs = jnp.swapaxes(layer_input, 0, 1).astype(jnp.float32)
    cotangent = jnp.swapaxes(output_cotangent, 0, 1)
    cos_table, sine_table = half_tables(length)
    own_cos = lax.dynamic_slice_in_dim(cos_table, ctx_index * block_len, block_len, 1)
    own_sine = lax.dynamic_slice_in_dim(sine_table, ctx_index * block_len, block_len, 1)
    prefix = lax.dynamic_slice_in_dim(prefix_len, ctx_index * seq_count // places, 1, 0)
    normed_low = norm_rows(inputs, attn_scale).astype(low)
    blocks_shape = (places, features, block_len)

    def project(matrix, rotated):
        product = matmul("bsd,de->bes", normed_low, matrix)
        if rotated:
            heads = product.reshape(seq_count, local // HEAD_DIM, 2, HEAD_DIM // 2, block_len)
            first, second = heads[:, :, 0], heads[:, :, 1]
            product = jnp.stack(
                [first * own_cos - second * own_sine, second * own_cos + first * own_sine], axis=2
            )
        return product.astype(low).reshape(blocks_shape)

    *blocks, mixed_low, log_total, full_gate, full_up, full_down = attend(
        project(full_query, True),
        project(full_key, True),
        project(full_value, False),
        shards[5:],
        prefix,
        2,
    )
    mixed_low = mixed_low.reshape(seq_count, local, block_len)
    hidden = inputs + both_cores(matmul("bes,de->bsd", mixed_low, full_out))
    hnorm_low = norm_rows(hidden, mlp_scale).astype(low)
    gate_out = matmul("bsd,df->bsf", hnorm_low, full_gate)
    up_out = matmul("bsd,df->bsf", hnorm_low, full_up)
    gate_sigmoid = jax.nn.sigmoid(gate_out)
    silu = gate_out * gate_sigmoid
    activated = (silu * up_out).astype(low)
    layer_output = (hidden + both_cores(matmul("bsf,df->bsd", activated, full_down))).astype(low)
    down_w_grad = matmul("bsd,bsf->df", cotangent, activated)
    act_grad = matmul("bsd,df->bsf", cotangent, full_down)
    gate_grad = (
        act_grad * up_out * (gate_sigmoid * (1.0 + gate_out * (1.0 - gate_sigmoid)))
    ).astype(low)
    up_grad = (act_grad * silu).astype(low)
    hnorm_part = matmul("bsf,df->bsd", gate_grad, full_gate) + matmul(
        "bsf,df->bsd", up_grad, full_up
    )
    hnorm_grad = both_cores(hnorm_part)
    gate_w_grad = matmul("bsd,bsf->df", hnorm_low, gate_grad)
    up_w_grad = matmul("bsd,bsf->df", hnorm_low, up_grad)
    hidden_back, mlp_gain_part = norm_back(hidden, mlp_scale, hnorm_grad)
    hidden_grad = cotangent.astype(jnp.float32) + hidden_back
    hidden_low = hidden_grad.astype(low)
    attn_grad = matmul("bsd,de->bes", hidden_low, full_out).astype(low)
    out_w_grad = matmul("bsd,bes->de", hidden_low, mixed_low)
    *grads, down, gate, up, out = attend_back_heads(
        attn_grad.reshape(blocks_shape),
        blocks,
        log_total,
        prefix,
        cos_table,
        sine_table,
        [grad.astype(low) for grad in (down_w_grad, gate_w_grad, up_w_grad, out_w_grad)],
        3,
    )
    grads = [grad.reshape(seq_count, local, block_len) for grad in grads]
    normed_part = (
        matmul("bes,de->bsd", grads[0], full_query)
        + matmul("bes,de->bsd", grads[1], full_key)
        + matmul("bes,de->bsd", grads[2], full_value)
    )
    normed_grad = both_cores(normed_part)
    input_back, attn_gain_part = norm_back(inputs, attn_scale, normed_grad)
    input_grad = (hidden_grad + input_back).astype(low)
    weight_grads = [
        matmul("bsd,bes->de", normed_low, grads[0]),
        matmul("bsd,bes->de", normed_low, grads[1]),
        matmul("bsd,bes->de", normed_low, grads[2]),
    ]
    count = lax.axis_size("fsdp")
    gain_parts = jax.vmap(gains_in)(
        attn_gain_part.reshape(count, -1), mlp_gain_part.reshape(count, -1)
    ).reshape(-1, 128)
    reduced = reduce_grads([gain_parts] + [grad.astype(low) for grad in weight_grads], 4)
    gains, query, key, value, down, gate, up, out = [
        total.astype(jnp.float32) for total in (*reduced, down, gate, up, out)
    ]
    return (
        jnp.swapaxes(layer_output, 0, 1),
        jnp.swapaxes(input_grad, 0, 1),
        gains_out(gains, 0, quarter),
        gains_out(gains, 1, quarter),
        query,
        key,
        value,
        out.T,
        gate,
        up,
        down.T,
    )


def heads_divide(mesh, args):
    block_rows = args[0].shape[0] // mesh.shape["ctx"]
    seqs = args[0].shape[1] // mesh.shape["fsdp"]
    heads = args[5].shape[1] // mesh.shape["tp"] // HEAD_DIM
    places = mesh.shape["ctx"]
    return (
        places == 4
        and mesh.shape["fsdp"] > 1
        and places % seqs == 0
        and heads % (places // seqs) == 0
        and block_rows % 256 == 0
    )


def solution(mesh):
    placed = (
        P("ctx", "fsdp", None),
        P("ctx", "fsdp", None),
        P("fsdp"),
        P("fsdp"),
        P("fsdp"),
        P("fsdp", "tp"),
        P("fsdp", "tp"),
        P("fsdp", "tp"),
        P("tp", "fsdp"),
        P("fsdp", "tp"),
        P("fsdp", "tp"),
        P("tp", "fsdp"),
    )
    def step(*args):
        chosen = heads_body if heads_divide(mesh, args) else body
        return spread_over(chosen)(*args)

    def spread_over(chosen):
      return jax.shard_map(
        chosen,
        mesh=mesh,
        in_specs=placed,
        out_specs=(
            P("ctx", "fsdp", None),
            P("ctx", "fsdp", None),
            P("fsdp"),
            P("fsdp"),
            P("fsdp", "tp"),
            P("fsdp", "tp"),
            P("fsdp", "tp"),
            P("tp", "fsdp"),
            P("fsdp", "tp"),
            P("fsdp", "tp"),
            P("tp", "fsdp"),
        ),
        check_vma=False,
    )

    return step
```

```python
import functools
import math

import jax
import jax.numpy as jnp
from jax import lax
from jax.experimental import pallas as pl
from jax.experimental.pallas import tpu as pltpu
from jax.sharding import PartitionSpec as P

HEAD_DIM = 64


EPS = 1e-06
BASE = 10000.0
MASKED = -1e30


def partner(block, axis, apart):
    count = lax.axis_size(axis)
    route = []
    for low in range(count):
        high = low | 1 << apart
        if high != low and high < count:
            route += [(low, high), (high, low)]
    return lax.ppermute(block, axis, route)


def from_behind(value, axis, steps):
    count = lax.axis_size(axis)
    pairs = [(source, (source + steps) % count) for source in range(count)]
    return lax.ppermute(value, axis, pairs)


def norm_rows(values, gain):
    return values * lax.rsqrt(jnp.mean(values * values, axis=-1, keepdims=True) + EPS) * gain


def rope_tables(positions):
    half_dim = HEAD_DIM // 2
    frequency = jnp.exp(
        jnp.arange(half_dim, dtype=jnp.float32) * (-2.0 * math.log(BASE) / HEAD_DIM)
    )
    angles = positions.astype(jnp.float32)[:, None] * frequency[None, :]
    cos_table = jnp.concatenate([jnp.cos(angles), jnp.cos(angles)], axis=1)
    sine_table = jnp.concatenate([jnp.sin(angles), jnp.sin(angles)], axis=1)
    return (cos_table[:, None, None, :], sine_table[:, None, None, :])


def rotary(values, cos_table, sine_table):
    half_dim = values.shape[-1] // 2
    turned = jnp.concatenate([-values[..., half_dim:], values[..., :half_dim]], axis=-1)
    return values * cos_table + turned * sine_table


def unrotary(grads, cos_table, sine_table):
    half_dim = grads.shape[-1] // 2
    scaled = grads * sine_table
    turned = jnp.concatenate([scaled[..., half_dim:], -scaled[..., :half_dim]], axis=-1)
    return grads * cos_table + turned


def block_positions(device, block_len, ctx_size):
    half_len = block_len // 2
    steps = jnp.arange(half_len, dtype=jnp.int32)
    first_part = 2 * device * half_len + steps
    second_part = (2 * ctx_size - 1 - 2 * device) * half_len + steps
    return jnp.concatenate([first_part, second_part], axis=0)


def mirror_rows(values):
    ctx_bits = lax.axis_size("ctx").bit_length() - 1
    for bit in range(ctx_bits):
        values = partner(values, "ctx", bit)
    return values


def visible(prefix_len, query_pos, key_pos):
    causal = key_pos[None, :] <= query_pos[:, None]
    opened = key_pos[None, None, :] < prefix_len[:, None, None]
    return (causal[None] | opened)[:, None]


def block_needed(prefix_len, query_pos, key_pos):
    first_key = jnp.min(key_pos)
    return (first_key <= jnp.max(query_pos)) | jnp.any(prefix_len > first_key)


def attend_step(softmax_state, queries, key_value, prefix_len, query_pos, key_pos):
    key_heads = key_value[..., :HEAD_DIM]
    value_heads = key_value[..., HEAD_DIM:]

    def compute(state_in):
        row_max, row_sum, weighted = state_in
        scores = jnp.einsum(
            "qshd,kshd->shqk", queries, key_heads, preferred_element_type=jnp.float32
        ) * HEAD_DIM ** (-0.5)
        allowed = visible(prefix_len, query_pos, key_pos)
        block_max = jnp.max(jnp.where(allowed, scores, MASKED), axis=-1)
        fresh_max = jnp.maximum(row_max, block_max)
        exps = jnp.where(allowed, jnp.exp(scores - fresh_max[..., None]), 0.0)
        factor = jnp.exp(row_max - fresh_max)
        row_sum = row_sum * factor + jnp.sum(exps, axis=-1)
        weighted = weighted * jnp.transpose(factor, (2, 0, 1))[..., None] + jnp.einsum(
            "shqk,kshd->qshd",
            exps.astype(jnp.bfloat16),
            value_heads,
            preferred_element_type=jnp.float32,
        )
        return (fresh_max, row_sum, weighted)

    def skipped(state_in):
        return state_in

    return lax.cond(block_needed(prefix_len, query_pos, key_pos), compute, skipped, softmax_state)


def attend_back(
    queries, attn_grad, log_total, delta_rows, key_value, prefix_len, query_pos, key_pos
):
    key_heads = key_value[..., :HEAD_DIM]
    value_heads = key_value[..., HEAD_DIM:]
    score_scale = HEAD_DIM ** (-0.5)

    def compute(unused):
        scores = (
            jnp.einsum("qshd,kshd->shqk", queries, key_heads, preferred_element_type=jnp.float32)
            * score_scale
        )
        allowed = visible(prefix_len, query_pos, key_pos)
        probabilities = jnp.where(allowed, jnp.exp(scores - log_total[..., None]), 0.0)
        prob_grad = jnp.einsum(
            "qshd,kshd->shqk", attn_grad, value_heads, preferred_element_type=jnp.float32
        )
        score_grad = (probabilities * (prob_grad - delta_rows[..., None])).astype(jnp.bfloat16)
        query_part = (
            jnp.einsum("shqk,kshd->qshd", score_grad, key_heads, preferred_element_type=jnp.float32)
            * score_scale
        )
        key_part = (
            jnp.einsum("shqk,qshd->kshd", score_grad, queries, preferred_element_type=jnp.float32)
            * score_scale
        )
        value_part = jnp.einsum(
            "shqk,qshd->kshd",
            probabilities.astype(jnp.bfloat16),
            attn_grad,
            preferred_element_type=jnp.float32,
        )
        return (query_part, jnp.concatenate([key_part, value_part], axis=-1))

    def skipped(unused):
        return (jnp.zeros(queries.shape, jnp.float32), jnp.zeros(key_value.shape, jnp.float32))

    return lax.cond(block_needed(prefix_len, query_pos, key_pos), compute, skipped, 0)


def pass_grads(key_grads):
    return from_behind(key_grads.astype(jnp.bfloat16), "ctx", 1).astype(key_grads.dtype)


def body(
    layer_input,
    output_cotangent,
    prefix_len,
    attn_gain,
    mlp_gain,
    query_weight,
    key_weight,
    value_weight,
    out_weight,
    gate_weight,
    up_weight,
    down_weight,
):
    block_len, seq_count, width = layer_input.shape
    half_len = block_len // 2
    ctx_size = lax.axis_size("ctx")
    ctx_index = lax.axis_index("ctx")
    moved = mirror_rows(jnp.stack([layer_input[half_len:], output_cotangent[half_len:]], axis=0))
    layer_input = jnp.concatenate([layer_input[:half_len], moved[0]], axis=0)
    output_cotangent = jnp.concatenate([output_cotangent[:half_len], moved[1]], axis=0)
    query_pos = block_positions(ctx_index, block_len, ctx_size)
    cos_table, sine_table = rope_tables(query_pos)
    gain_one, full_query, full_key, full_value, full_out = (
        lax.all_gather(attn_gain.astype(jnp.bfloat16), "fsdp", axis=0, tiled=True),
        lax.all_gather(query_weight.astype(jnp.bfloat16), "fsdp", axis=0, tiled=True),
        lax.all_gather(key_weight.astype(jnp.bfloat16), "fsdp", axis=0, tiled=True),
        lax.all_gather(value_weight.astype(jnp.bfloat16), "fsdp", axis=0, tiled=True),
        lax.all_gather(out_weight.astype(jnp.bfloat16), "fsdp", axis=1, tiled=True),
    )
    gain_two, full_gate, full_up, full_down = (
        lax.all_gather(mlp_gain.astype(jnp.bfloat16), "fsdp", axis=0, tiled=True),
        lax.all_gather(gate_weight.astype(jnp.bfloat16), "fsdp", axis=0, tiled=True),
        lax.all_gather(up_weight.astype(jnp.bfloat16), "fsdp", axis=0, tiled=True),
        lax.all_gather(down_weight.astype(jnp.bfloat16), "fsdp", axis=1, tiled=True),
    )
    heads_local = full_query.shape[1] // HEAD_DIM
    inputs = layer_input.astype(jnp.float32)
    attn_scale = gain_one.astype(jnp.float32)
    normed_low = norm_rows(inputs, attn_scale).astype(jnp.bfloat16)

    def project(matrix):
        product = jnp.einsum("bsd,de->bse", normed_low, matrix, preferred_element_type=jnp.float32)
        return product.reshape(block_len, seq_count, heads_local, HEAD_DIM)

    queries = rotary(project(full_query), cos_table, sine_table).astype(jnp.bfloat16)
    key_heads = rotary(project(full_key), cos_table, sine_table).astype(jnp.bfloat16)
    value_heads = project(full_value).astype(jnp.bfloat16)
    key_value = jnp.concatenate([key_heads, value_heads], axis=-1)
    stats_shape = (seq_count, heads_local, block_len)
    initial = (
        jnp.full(stats_shape, MASKED, jnp.float32),
        jnp.zeros(stats_shape, jnp.float32),
        jnp.zeros((block_len, seq_count, heads_local, HEAD_DIM), jnp.float32),
    )
    softmax_state = attend_step(initial, queries, key_value, prefix_len, query_pos, query_pos)

    def forward_shift(counter, loop_carry):
        state_in, moving = loop_carry
        moving = from_behind(moving, "ctx", 1)
        source = (ctx_index - counter) % ctx_size
        key_pos = block_positions(source, block_len, ctx_size)
        state_in = attend_step(state_in, queries, moving, prefix_len, query_pos, key_pos)
        return (state_in, moving)

    softmax_state, unused_keys = lax.fori_loop(
        1, ctx_size, forward_shift, (softmax_state, key_value)
    )
    row_max, row_sum, weighted = softmax_state
    log_total = row_max + jnp.log(row_sum)
    attn_exact = weighted / jnp.transpose(row_sum, (2, 0, 1))[..., None]
    mixed_low = attn_exact.reshape(block_len, seq_count, heads_local * HEAD_DIM).astype(
        jnp.bfloat16
    )
    attn_part = jnp.einsum("bse,ed->bsd", mixed_low, full_out, preferred_element_type=jnp.float32)
    hidden = inputs + lax.psum(attn_part.astype(jnp.bfloat16), "tp").astype(jnp.float32)
    mlp_scale = gain_two.astype(jnp.float32)
    hnorm_low = norm_rows(hidden, mlp_scale).astype(jnp.bfloat16)
    gate_out = jnp.einsum("bsd,df->bsf", hnorm_low, full_gate, preferred_element_type=jnp.float32)
    up_out = jnp.einsum("bsd,df->bsf", hnorm_low, full_up, preferred_element_type=jnp.float32)
    activated = (jax.nn.silu(gate_out) * up_out).astype(jnp.bfloat16)
    down_part = jnp.einsum("bsf,fd->bsd", activated, full_down, preferred_element_type=jnp.float32)
    result = hidden + lax.psum(down_part.astype(jnp.bfloat16), "tp").astype(jnp.float32)
    layer_output = result.astype(jnp.bfloat16)
    grad_float = output_cotangent.astype(jnp.float32)
    down_w_grad = jnp.einsum(
        "bsf,bsd->fd", activated, output_cotangent, preferred_element_type=jnp.float32
    )
    act_grad = jnp.einsum(
        "bsd,fd->bsf", output_cotangent, full_down, preferred_element_type=jnp.float32
    )
    unused_value, silu_pullback = jax.vjp(
        lambda gate_in, up_in: jax.nn.silu(gate_in) * up_in, gate_out, up_out
    )
    gate_back, up_back = silu_pullback(act_grad)
    gate_grad = gate_back.astype(jnp.bfloat16)
    up_grad = up_back.astype(jnp.bfloat16)
    gate_w_grad = jnp.einsum(
        "bsd,bsf->df", hnorm_low, gate_grad, preferred_element_type=jnp.float32
    )
    up_w_grad = jnp.einsum("bsd,bsf->df", hnorm_low, up_grad, preferred_element_type=jnp.float32)
    hnorm_part = jnp.einsum(
        "bsf,df->bsd", gate_grad, full_gate, preferred_element_type=jnp.float32
    ) + jnp.einsum("bsf,df->bsd", up_grad, full_up, preferred_element_type=jnp.float32)
    hnorm_grad = lax.psum(hnorm_part.astype(jnp.bfloat16), "tp").astype(jnp.float32)
    unused_norm, norm_pullback = jax.vjp(norm_rows, hidden, mlp_scale)
    hidden_back, mlp_gain_part = norm_pullback(hnorm_grad)
    hidden_grad = grad_float + hidden_back
    hidden_low = hidden_grad.astype(jnp.bfloat16)
    out_w_grad = jnp.einsum(
        "bse,bsd->ed", mixed_low, hidden_low, preferred_element_type=jnp.float32
    )
    attn_grad = jnp.einsum(
        "bsd,ed->bse", hidden_low, full_out, preferred_element_type=jnp.float32
    ).astype(jnp.bfloat16)
    attn_grad = attn_grad.reshape(block_len, seq_count, heads_local, HEAD_DIM)
    delta_rows = jnp.transpose(
        jnp.sum(attn_grad.astype(jnp.float32) * attn_exact, axis=-1), (1, 2, 0)
    )
    zero_query = jnp.zeros((block_len, seq_count, heads_local, HEAD_DIM), jnp.float32)

    def backward_shift(counter, loop_carry):
        query_acc, moving, travelling = loop_carry
        source = (ctx_index - counter) % ctx_size
        key_pos = block_positions(source, block_len, ctx_size)
        query_part, key_part = attend_back(
            queries, attn_grad, log_total, delta_rows, moving, prefix_len, query_pos, key_pos
        )
        travelling = pass_grads(travelling + key_part)
        moving = from_behind(moving, "ctx", 1)
        return (query_acc + query_part, moving, travelling)

    travel_zero = jnp.zeros((block_len, seq_count, heads_local, 2 * HEAD_DIM), jnp.float32)
    query_acc, moving, travelling = lax.fori_loop(
        0, ctx_size - 1, backward_shift, (zero_query, key_value, travel_zero)
    )
    last_source = (ctx_index + 1) % ctx_size
    last_pos = block_positions(last_source, block_len, ctx_size)
    query_part, key_part = attend_back(
        queries, attn_grad, log_total, delta_rows, moving, prefix_len, query_pos, last_pos
    )
    query_acc = query_acc + query_part
    own_grads = pass_grads(travelling + key_part)
    flat_shape = (block_len, seq_count, heads_local * HEAD_DIM)
    query_grad = unrotary(query_acc, cos_table, sine_table).astype(jnp.bfloat16).reshape(flat_shape)
    key_grad = (
        unrotary(own_grads[..., :HEAD_DIM], cos_table, sine_table)
        .astype(jnp.bfloat16)
        .reshape(flat_shape)
    )
    value_grad = own_grads[..., HEAD_DIM:].astype(jnp.bfloat16).reshape(flat_shape)
    query_w_grad = jnp.einsum(
        "bsd,bse->de", normed_low, query_grad, preferred_element_type=jnp.float32
    )
    key_w_grad = jnp.einsum("bsd,bse->de", normed_low, key_grad, preferred_element_type=jnp.float32)
    value_w_grad = jnp.einsum(
        "bsd,bse->de", normed_low, value_grad, preferred_element_type=jnp.float32
    )
    normed_part = (
        jnp.einsum("bse,de->bsd", query_grad, full_query, preferred_element_type=jnp.float32)
        + jnp.einsum("bse,de->bsd", key_grad, full_key, preferred_element_type=jnp.float32)
        + jnp.einsum("bse,de->bsd", value_grad, full_value, preferred_element_type=jnp.float32)
    )
    normed_grad = lax.psum(normed_part.astype(jnp.bfloat16), "tp").astype(jnp.float32)
    unused_first, first_pullback = jax.vjp(norm_rows, inputs, attn_scale)
    input_back, attn_gain_part = first_pullback(normed_grad)
    input_grad = (hidden_grad + input_back).astype(jnp.bfloat16)
    returned = mirror_rows(jnp.stack([layer_output[half_len:], input_grad[half_len:]], axis=0))
    layer_output = jnp.concatenate([layer_output[:half_len], returned[0]], axis=0)
    input_grad = jnp.concatenate([input_grad[:half_len], returned[1]], axis=0)
    shards = (
        lax.psum_scatter(
            attn_gain_part.astype(jnp.bfloat16), "fsdp", scatter_dimension=0, tiled=True
        ).astype(jnp.float32),
        lax.psum_scatter(
            mlp_gain_part.astype(jnp.bfloat16), "fsdp", scatter_dimension=0, tiled=True
        ).astype(jnp.float32),
        lax.psum_scatter(
            query_w_grad.astype(jnp.bfloat16), "fsdp", scatter_dimension=0, tiled=True
        ).astype(jnp.float32),
        lax.psum_scatter(
            key_w_grad.astype(jnp.bfloat16), "fsdp", scatter_dimension=0, tiled=True
        ).astype(jnp.float32),
        lax.psum_scatter(
            value_w_grad.astype(jnp.bfloat16), "fsdp", scatter_dimension=0, tiled=True
        ).astype(jnp.float32),
        lax.psum_scatter(
            out_w_grad.astype(jnp.bfloat16), "fsdp", scatter_dimension=1, tiled=True
        ).astype(jnp.float32),
        lax.psum_scatter(
            gate_w_grad.astype(jnp.bfloat16), "fsdp", scatter_dimension=0, tiled=True
        ).astype(jnp.float32),
        lax.psum_scatter(
            up_w_grad.astype(jnp.bfloat16), "fsdp", scatter_dimension=0, tiled=True
        ).astype(jnp.float32),
        lax.psum_scatter(
            down_w_grad.astype(jnp.bfloat16), "fsdp", scatter_dimension=1, tiled=True
        ).astype(jnp.float32),
    )
    totals = (
        lax.psum(shards[0].astype(jnp.bfloat16), "ctx").astype(jnp.float32),
        lax.psum(shards[1].astype(jnp.bfloat16), "ctx").astype(jnp.float32),
        lax.psum(shards[2].astype(jnp.bfloat16), "ctx").astype(jnp.float32),
        lax.psum(shards[3].astype(jnp.bfloat16), "ctx").astype(jnp.float32),
        lax.psum(shards[4].astype(jnp.bfloat16), "ctx").astype(jnp.float32),
        lax.psum(shards[5].astype(jnp.bfloat16), "ctx").astype(jnp.float32),
        lax.psum(shards[6].astype(jnp.bfloat16), "ctx").astype(jnp.float32),
        lax.psum(shards[7].astype(jnp.bfloat16), "ctx").astype(jnp.float32),
        lax.psum(shards[8].astype(jnp.bfloat16), "ctx").astype(jnp.float32),
    )
    return (
        layer_output,
        input_grad,
        totals[0],
        totals[1],
        totals[2],
        totals[3],
        totals[4],
        totals[5],
        totals[6],
        totals[7],
        totals[8],
    )


MESH = pl.DeviceIdType.MESH
VMEM_LIMIT = 60 << 20
LINE = 2


def place():
    ctx = lax.axis_index("ctx")
    along_x = ctx + 1 - 2 * lax.rem(ctx, 2)
    along_y = lax.rem(ctx + 2, 4)
    return lax.axis_index("fsdp"), ctx, along_x, along_y, 3 - ctx


def greet(devices):
    barrier = pltpu.get_barrier_semaphore()
    for device in devices:
        pl.semaphore_signal(barrier, inc=1, device_id=device, device_id_type=MESH)
    pl.semaphore_wait(barrier, len(devices))


def rows_at(block, rows):
    return pl.ds(pl.multiple_of(block * rows, 16), rows)


def send(source, target, send_sem, recv_sem, device):
    return pltpu.make_async_remote_copy(
        src_ref=source,
        dst_ref=target,
        send_sem=send_sem,
        recv_sem=recv_sem,
        device_id=device,
        device_id_type=MESH,
    )


def column_chunks(shapes, widest, paths=2):
    chunks = []
    for index, (rows, columns) in enumerate(shapes):
        count = -(-columns // widest)
        while columns % count or (columns // count) % 128:
            count += 1
        width = columns // count
        chunks += [(index, rows // 4, part * width, width) for part in range(count)]
    return [chunk + (number % paths,) for number, chunk in enumerate(chunks)]


def gather_steps(chunks, shard_refs, full_refs, local_sem, send_sems, recv_sems):
    fsdp, ctx, along_x, along_y, across = place()
    last = lax.axis_size("fsdp") - 1

    def region(chunk, shard, quarter):
        index, rows, low, width, path = chunk
        if path == LINE:
            return full_refs[index].at[rows_at(shard, 4 * rows), pl.ds(low, width)]
        return full_refs[index].at[rows_at(shard * 4 + quarter, rows), pl.ds(low, width)]

    def pass_on(number, shard, quarter, kind, device, source=None):
        target = region(chunks[number], shard, quarter)
        return send(
            target if source is None else source,
            target,
            send_sems.at[number, shard, kind],
            recv_sems.at[number, shard, quarter],
            device,
        )

    def own_source(number):
        index, rows, low, width, path = chunks[number]
        if path == LINE:
            return shard_refs[index].at[:, pl.ds(low, width)]
        return shard_refs[index].at[rows_at(ctx, rows), pl.ds(low, width)]

    def arrived(number, shard, quarter):
        pass_on(number, shard, quarter, 0, {"ctx": along_x}).wait_recv()

    count = range(len(chunks))
    up, down = {"fsdp": lax.rem(fsdp + 1, last + 1)}, {"fsdp": lax.rem(fsdp + last, last + 1)}
    to_x, to_y = {"ctx": along_x}, {"ctx": along_y}

    def begin():
        for number in count:

            @pl.when(fsdp < last)
            def _(number=number):
                pass_on(number, fsdp, ctx, 0, up, own_source(number)).start()

            @pl.when(fsdp > 0)
            def _(number=number):
                pass_on(number, fsdp, ctx, 1, down, own_source(number)).start()

        for index, shard_ref in enumerate(shard_refs):
            rows = shard_ref.shape[0]
            pltpu.make_async_copy(
                shard_ref, full_refs[index].at[rows_at(fsdp, rows)], local_sem.at[index]
            ).start()

    def each(steps, act):
        for sign in (-1, 1):
            shard = fsdp + sign * steps

            @pl.when((shard >= 0) & (shard <= last))
            def _(sign=sign, shard=shard):
                act(shard, sign)

    def from_line(number, steps):
        def act(shard, sign):
            arrived(number, shard, ctx)
            if sign < 0:

                @pl.when(fsdp < last)
                def _():
                    pass_on(number, shard, ctx, 0, up).start()

            else:

                @pl.when(fsdp > 0)
                def _():
                    pass_on(number, shard, ctx, 1, down).start()

            if chunks[number][-1] != LINE:
                pass_on(number, shard, ctx, 2, to_x).start()
                pass_on(number, shard, ctx, 3, to_y).start()

        each(steps, act)

    def to_corner(number, steps):
        if chunks[number][-1] == LINE:
            return

        def act(shard, sign):
            if chunks[number][-1] == 0:
                arrived(number, shard, along_x)
                pass_on(number, shard, along_x, 4, to_y).start()
            else:
                arrived(number, shard, along_y)
                pass_on(number, shard, along_y, 4, to_x).start()

        each(steps, act)

    def finish():
        for steps in range(1, last + 1):
            for number in count:

                def act(shard, sign, number=number):
                    if chunks[number][-1] != LINE:
                        arrived(number, shard, along_y if chunks[number][-1] == 0 else along_x)
                        arrived(number, shard, across)
                    forward = fsdp < last if sign < 0 else fsdp > 0

                    @pl.when(forward)
                    def _():
                        pass_on(number, shard, ctx, 0 if sign < 0 else 1, up).wait_send()

                    if chunks[number][-1] != LINE:
                        for kind in (2, 3, 4):
                            pass_on(number, shard, ctx, kind, to_x).wait_send()

                each(steps, act)
        for number in count:

            @pl.when(fsdp < last)
            def _(number=number):
                pass_on(number, fsdp, ctx, 0, up, own_source(number)).wait_send()

            @pl.when(fsdp > 0)
            def _(number=number):
                pass_on(number, fsdp, ctx, 1, down, own_source(number)).wait_send()

        for index, shard_ref in enumerate(shard_refs):
            rows = shard_ref.shape[0]
            pltpu.make_async_copy(
                shard_ref, full_refs[index].at[rows_at(fsdp, rows)], local_sem.at[index]
            ).wait()

    return begin, from_line, to_corner, finish


def neighbours(fsdp, along_x, along_y):
    size = lax.axis_size("fsdp")
    return [
        {"ctx": along_x},
        {"ctx": along_y},
        {"fsdp": lax.rem(fsdp + 1, size)},
        {"fsdp": lax.rem(fsdp + size - 1, size)},
    ]


def gather_kernel(chunks, arrays, *refs):
    shard_refs, full_refs = refs[:arrays], refs[arrays : 2 * arrays]
    local_sem, send_sems, recv_sems = refs[2 * arrays :]
    fsdp, ctx, along_x, along_y, across = place()
    greet(neighbours(fsdp, along_x, along_y))
    begin, from_line, to_corner, finish = gather_steps(
        chunks, shard_refs, full_refs, local_sem, send_sems, recv_sems
    )
    begin()
    last = lax.axis_size("fsdp") - 1
    for steps in range(1, last + 2):
        for number in range(len(chunks)):
            if steps <= last:
                from_line(number, steps)
            if steps > 1:
                to_corner(number, steps - 1)
    finish()


def gather_scratch(shards, chunks):
    return [
        pltpu.SemaphoreType.DMA((len(shards),)),
        pltpu.SemaphoreType.DMA((len(chunks), 4, 5)),
        pltpu.SemaphoreType.DMA((len(chunks), 4, 4)),
    ]


def gather_shards(shards, collective_id):
    chunks = column_chunks([shard.shape for shard in shards], 128)
    size = lax.axis_size("fsdp")
    anywhere = pl.BlockSpec(memory_space=pl.ANY)
    return pl.pallas_call(
        functools.partial(gather_kernel, chunks, len(shards)),
        out_shape=[
            jax.ShapeDtypeStruct((size * shard.shape[0], shard.shape[1]), shard.dtype)
            for shard in shards
        ],
        in_specs=[pl.BlockSpec(memory_space=pltpu.VMEM)] * len(shards),
        out_specs=[anywhere] * len(shards),
        scratch_shapes=gather_scratch(shards, chunks),
        compiler_params=pltpu.CompilerParams(
            collective_id=collective_id, has_side_effects=True, vmem_limit_bytes=VMEM_LIMIT
        ),
        name="gather_shards",
    )(*shards)


def reduce_steps(chunks, full_refs, out_refs, rest):
    count = len(chunks)
    buffers = [rest[6 * number : 6 * number + 6] for number in range(count)]
    load_sems, send_sems, recv_sems = rest[6 * count :]
    fsdp, ctx, along_x, along_y, across = place()
    size = lax.axis_size("fsdp")
    others = [{"fsdp": lax.rem(fsdp + step, size)} for step in range(1, size)]

    def quarter_of(number, quarter):
        index, rows, low, width, _ = chunks[number]
        return full_refs[index].at[:, rows_at(quarter, rows), pl.ds(low, width)]

    def result(number, quarter):
        index, rows, low, width, _ = chunks[number]
        return out_refs[index].at[rows_at(quarter, rows), pl.ds(low, width)]

    def first_second(number):
        return (along_x, along_y) if chunks[number][-1] == 0 else (along_y, along_x)

    def exchange(number, part):
        first, _ = first_second(number)
        return send(
            quarter_of(number, first if part == 0 else across),
            buffers[number][1].at[part],
            send_sems.at[number, part],
            recv_sems.at[number, part],
            {"ctx": first},
        )

    def load(number, part):
        _, second = first_second(number)
        return pltpu.make_async_copy(
            quarter_of(number, ctx if part == 0 else second),
            buffers[number][0].at[part],
            load_sems.at[number, part],
        )

    def second_hop(number):
        _, second = first_second(number)
        return send(
            buffers[number][2],
            buffers[number][3],
            send_sems.at[number, 2],
            recv_sems.at[number, 2],
            {"ctx": second},
        )

    def along_line(number, step):
        return send(
            buffers[number][4].at[lax.rem(fsdp + step, size)],
            buffers[number][5].at[step - 1],
            send_sems.at[number, 2 + step],
            recv_sems.at[number, 2 + step],
            others[step - 1],
        )

    def spread(number, quarter, kind, target):
        place_there = result(number, quarter)
        return send(
            place_there,
            place_there,
            send_sems.at[number, 2 + size + kind],
            recv_sems.at[number, 2 + size + kind],
            {"ctx": target},
        )

    def stage(number, at):
        first, second = first_second(number)
        own, landed, passing, arrived, total, line = buffers[number]
        if at == 0:
            for part in (1, 0):
                exchange(number, part).start()
                load(number, part).start()
        elif at == 1:
            load(number, 1).wait()
            exchange(number, 1).wait_recv()
            passing[...] = (own[1].astype(jnp.float32) + landed[1].astype(jnp.float32)).astype(
                jnp.bfloat16
            )
            second_hop(number).start()
        elif at == 2:
            load(number, 0).wait()
            exchange(number, 0).wait_recv()
            second_hop(number).wait_recv()
            total[...] = (
                own[0].astype(jnp.float32)
                + landed[0].astype(jnp.float32)
                + arrived[...].astype(jnp.float32)
            ).astype(jnp.bfloat16)
            for step in range(1, size):
                along_line(number, step).start()
        elif at == 3:
            value = total[fsdp].astype(jnp.float32)
            for step in range(1, size):
                along_line(number, step).wait_recv()
                value = value + line[step - 1].astype(jnp.float32)
            index, rows, low, width, _ = chunks[number]
            out_refs[index][rows_at(ctx, rows), pl.ds(low, width)] = value.astype(jnp.bfloat16)
            spread(number, ctx, 0, first).start()
            spread(number, ctx, 1, second).start()
        elif at == 4:
            spread(number, first, 0, first).wait_recv()
            spread(number, first, 2, second).start()
        else:
            spread(number, second, 1, second).wait_recv()
            spread(number, across, 2, second).wait_recv()
            for part in (0, 1):
                exchange(number, part).wait_send()
            second_hop(number).wait_send()
            for step in range(1, size):
                along_line(number, step).wait_send()
            for kind in range(3):
                spread(number, ctx, kind, first).wait_send()

    return stage


def reduce_order(count, lag):
    return [
        (number, at)
        for tick in range(count + 4 * lag)
        for at in range(5, 0, -1)
        for number in (tick - (at - 1) * lag,)
        if 0 <= number < count
    ]


def close_by():
    fsdp, ctx, along_x, along_y, across = place()
    size = lax.axis_size("fsdp")
    return [{"ctx": along_x}, {"ctx": along_y}, {"ctx": across}] + [
        {"fsdp": lax.rem(fsdp + step, size)} for step in range(1, size)
    ]


def reduce_kernel(chunks, arrays, *refs):
    greet(close_by())
    stage = reduce_steps(chunks, refs[:arrays], refs[arrays : 2 * arrays], refs[2 * arrays :])
    for number in range(len(chunks)):
        stage(number, 0)
    for number, at in reduce_order(len(chunks), 2):
        stage(number, at)


def reduce_scratch(chunks, size):
    scratch = []
    for _, rows, _, width, _ in chunks:
        block = (size, rows, width)
        for shape in ((2,) + block, (2,) + block, block, block, block, (size - 1, rows, width)):
            scratch.append(pltpu.VMEM(shape, jnp.bfloat16))
    return scratch + [
        pltpu.SemaphoreType.DMA((len(chunks), 2)),
        pltpu.SemaphoreType.DMA((len(chunks), size + 5)),
        pltpu.SemaphoreType.DMA((len(chunks), size + 5)),
    ]


def reduce_grads(grads, collective_id):
    size = lax.axis_size("fsdp")
    shapes = [(grad.shape[0] // size, grad.shape[1]) for grad in grads]
    chunks = column_chunks(shapes, 128)
    anywhere = pl.BlockSpec(memory_space=pl.ANY)
    return pl.pallas_call(
        functools.partial(reduce_kernel, chunks, len(grads)),
        out_shape=[jax.ShapeDtypeStruct(shape, jnp.bfloat16) for shape in shapes],
        in_specs=[anywhere] * len(grads),
        out_specs=[pl.BlockSpec(memory_space=pltpu.VMEM)] * len(grads),
        scratch_shapes=reduce_scratch(chunks, size),
        compiler_params=pltpu.CompilerParams(
            collective_id=collective_id, has_side_effects=True, vmem_limit_bytes=VMEM_LIMIT
        ),
        name="reduce_grads",
    )(*[grad.reshape(size, shape[0], shape[1]) for grad, shape in zip(grads, shapes)])


def head_rows(head):
    return pl.ds(pl.multiple_of(head * HEAD_DIM, HEAD_DIM), HEAD_DIM)


def swap_steps(sources, landings, local_sems, send_sems, recv_sems):
    fsdp, ctx, along_x, along_y, across = place()
    targets = (across, along_x, along_y)

    def copies(head, local=True):
        rows = head_rows(head)
        made = []
        for index, (source, landing) in enumerate(zip(sources, landings)):
            for number, target in enumerate(targets):
                made.append(
                    send(
                        source.at[target, rows],
                        landing.at[ctx, rows],
                        send_sems.at[head, index, number],
                        recv_sems.at[head, index, number],
                        {"ctx": target},
                    )
                )
            if local:
                made.append(
                    pltpu.make_async_copy(
                        source.at[ctx, rows], landing.at[ctx, rows], local_sems.at[head, index]
                    )
                )
        return made

    def begin(head):
        for copy in copies(head):
            copy.start()

    def landed(head):
        for number, copy in enumerate(copies(head)):
            if number % 4 == 3:
                copy.wait()
            else:
                copy.wait_recv()

    def sent(head):
        for copy in copies(head, local=False):
            copy.wait_send()

    return begin, landed, sent


def swap_scratch(heads, arrays):
    return [
        pltpu.SemaphoreType.DMA((heads, arrays)),
        pltpu.SemaphoreType.DMA((heads, arrays, 3)),
        pltpu.SemaphoreType.DMA((heads, arrays, 3)),
    ]


def beside(head, slot, events):
    for at in sorted({event[0] for event in events if event[1] == slot}):

        @pl.when(head == at)
        def _(at=at):
            for planned, place_in, act in events:
                if planned == at and place_in == slot:
                    act()


def spaced(acts, slots, heads, first, gap):
    planned, left = [], []
    for number, act in enumerate(acts):
        at = first + int(number * gap)
        if at < slots * heads:
            planned.append((at // slots, at % slots, act))
        else:
            left.append(act)
    return planned, left


def dot(left, right):
    return jnp.dot(left, right, preferred_element_type=jnp.float32)


def turn(block):
    return block.astype(jnp.float32).T.astype(block.dtype)


def seen(prefix, row_block, key_block, rows, keys, values, fill):
    if (key_block + 1) * keys <= row_block * rows + 1:
        return values
    key_pos = key_block * keys + lax.broadcasted_iota(jnp.int32, values.shape, 1)
    row_pos = row_block * rows + lax.broadcasted_iota(jnp.int32, values.shape, 0)
    allowed = key_pos < jnp.maximum(row_pos + 1, prefix)
    return jnp.where(allowed, values, fill)


def key_blocks(row_block, rows, keys, length):
    farthest = max((row_block + 1) * rows, length // 2)
    return range(-(-farthest // keys))


def attend_kernel(rows, chunks, arrays, *refs):
    prefix_ref, query_in, key_in, value_in = refs[:4]
    shard_refs, refs = refs[4 : 4 + arrays], refs[4 + arrays :]
    query_blocks, key_blocks_ref, value_blocks, mixed_out, log_ref = refs[:5]
    full_refs, refs = refs[5 : 5 + arrays], refs[5 + arrays :]
    mixed_ref, query_ref, value_ref = refs[:3]
    fsdp, ctx, along_x, along_y, across = place()
    places, features, keys = query_in.shape
    heads = features // HEAD_DIM
    length = places * keys
    greet(close_by())
    begin, landed, sent = swap_steps(
        (query_in, key_in, value_in), (query_blocks, key_blocks_ref, value_blocks), *refs[3:6]
    )
    begin_back, landed_back, sent_back = swap_steps((mixed_ref,), (mixed_out,), *refs[6:9])
    begin_gather, from_line, to_corner, finish = gather_steps(
        chunks, shard_refs, full_refs, *refs[9:12]
    )
    for head in range(heads):
        begin(head)
    begin_gather()
    last = lax.axis_size("fsdp") - 1
    acts = []
    for steps in range(1, last + 2):
        for number in range(len(chunks)):
            if steps <= last:
                acts.append(functools.partial(from_line, number, steps))
            if steps > 1:
                acts.append(functools.partial(to_corner, number, steps - 1))
    slots = length // rows
    planned, left = spaced(acts, slots, heads, 1, slots * heads / len(acts))
    prefix = prefix_ref[0]

    @pl.loop(0, heads)
    def _(head):
        landed(head)
        inside_rows = head_rows(head)
        for block in range(places):
            span = pl.ds(block * keys, keys)
            query_ref[span, :] = turn(
                query_blocks[block, inside_rows] * jnp.bfloat16(HEAD_DIM ** (-0.5))
            )
            value_ref[span, :] = turn(value_blocks[block, inside_rows])
        for row_block in range(length // rows):
            span = pl.ds(row_block * rows, rows)
            queries = query_ref[span, :]
            scores = []
            for block in key_blocks(row_block, rows, keys, length):
                part = dot(queries, key_blocks_ref[block, inside_rows])
                scores.append(seen(prefix, row_block, block, rows, keys, part, MASKED))
            row_max = functools.reduce(
                jnp.maximum, [jnp.max(part, axis=1, keepdims=True) for part in scores]
            )
            row_sum = jnp.zeros_like(row_max)
            mixed = jnp.zeros((rows, HEAD_DIM), jnp.float32)
            for block, part in enumerate(scores):
                exps = jnp.exp(part - row_max)
                row_sum = row_sum + jnp.sum(exps, axis=1, keepdims=True)
                mixed = mixed + dot(
                    exps.astype(jnp.bfloat16), value_ref[pl.ds(block * keys, keys), :]
                )
            log_ref[head, span, :] = row_max + jnp.log(row_sum)
            block, inside = divmod(row_block * rows, keys)
            mixed_ref[block, inside_rows, pl.ds(inside, rows)] = (mixed / row_sum).T.astype(
                jnp.bfloat16
            )
            beside(head, row_block, planned)
        begin_back(head)

    for act in left:
        act()
    finish()
    for head in range(heads):
        landed_back(head)
        sent(head)
        sent_back(head)


def attend(query, key, value, shards, prefix, collective_id):
    places, features, keys = query.shape
    heads = features // HEAD_DIM
    length = places * keys
    size = lax.axis_size("fsdp")
    chunks = column_chunks([shard.shape for shard in shards], 512)
    chunks = [
        chunk[:-1] + (LINE if number % 2 else number // 2 % 2,)
        for number, chunk in enumerate(chunks)
    ]
    held = pl.BlockSpec(memory_space=pltpu.VMEM)
    anywhere = pl.BlockSpec(memory_space=pl.ANY)
    return pl.pallas_call(
        functools.partial(attend_kernel, min(256, keys), chunks, len(shards)),
        out_shape=[jax.ShapeDtypeStruct(query.shape, jnp.bfloat16)] * 4
        + [jax.ShapeDtypeStruct((heads, length, 1), jnp.float32)]
        + [
            jax.ShapeDtypeStruct((size * shard.shape[0], shard.shape[1]), shard.dtype)
            for shard in shards
        ],
        in_specs=[pl.BlockSpec(memory_space=pltpu.SMEM)] + [held] * (3 + len(shards)),
        out_specs=[held] * 3 + [anywhere, held] + [anywhere] * len(shards),
        scratch_shapes=[
            pltpu.VMEM(query.shape, jnp.bfloat16),
            pltpu.VMEM((length, HEAD_DIM), jnp.bfloat16),
            pltpu.VMEM((length, HEAD_DIM), jnp.bfloat16),
        ]
        + swap_scratch(heads, 3)
        + swap_scratch(heads, 1)
        + gather_scratch(shards, chunks),
        compiler_params=pltpu.CompilerParams(
            collective_id=collective_id, has_side_effects=True, vmem_limit_bytes=VMEM_LIMIT
        ),
        name="attend",
    )(prefix, query, key, value, *shards)


def turn_back(grads, cos_table, sine_table):
    half = HEAD_DIM // 2
    low, high = grads[:half], grads[half:]
    return (
        low * cos_table + high * sine_table,
        high * cos_table - low * sine_table,
    )


def attend_back_kernel(rows, chunks, arrays, *refs):
    prefix_ref, back_in, query_blocks, key_blocks_ref, value_blocks = refs[:5]
    log_ref, cos_ref, sine_ref = refs[5:8]
    weight_refs, refs = refs[8 : 8 + arrays], refs[8 + arrays :]
    landings, reduced_refs, refs = refs[:3], refs[3 : 3 + arrays], refs[3 + arrays :]
    back_ref, query_out, key_out, value_out = refs[:4]
    query_ref, key_ref, attn_ref, key_grad_ref, value_grad_ref = refs[4:9]
    places, features, keys = back_in.shape
    heads = features // HEAD_DIM
    length = places * keys
    half = HEAD_DIM // 2
    scale = HEAD_DIM ** (-0.5)
    greet(close_by())
    begin, landed, sent = swap_steps((back_in,), (back_ref,), *refs[9:12])
    begin_home, landed_home, sent_home = swap_steps(
        (query_out, key_out, value_out), landings, *refs[12:15]
    )
    stage = reduce_steps(chunks, weight_refs, reduced_refs, refs[15:])
    for head in range(heads):
        begin(head)
    for number in range(len(chunks)):
        stage(number, 0)
    acts = [functools.partial(stage, *step) for step in reduce_order(len(chunks), 2)]
    slots = length // rows
    planned, left = spaced(acts, slots, heads, 3, 1.2)
    prefix = prefix_ref[0]

    @pl.loop(0, heads)
    def _(head):
        landed(head)
        inside_rows = head_rows(head)
        for block in range(places):
            span = pl.ds(block * keys, keys)
            query_ref[span, :] = turn(query_blocks[block, inside_rows] * jnp.bfloat16(scale))
            key_ref[span, :] = turn(key_blocks_ref[block, inside_rows])
            attn_ref[span, :] = turn(back_ref[block, inside_rows])
        key_grad_ref[...] = jnp.zeros_like(key_grad_ref)
        value_grad_ref[...] = jnp.zeros_like(value_grad_ref)
        low_rows = pl.ds(pl.multiple_of(head * HEAD_DIM, half), half)
        high_rows = pl.ds(pl.multiple_of(head * HEAD_DIM + half, half), half)
        for row_block in range(length // rows):
            span = pl.ds(row_block * rows, rows)
            home, inside = divmod(row_block * rows, keys)
            lanes = pl.ds(inside, rows)
            queries, attn_grad = query_ref[span, :], attn_ref[span, :]
            queries_low = query_blocks[home, inside_rows, lanes] * jnp.bfloat16(scale)
            attn_low = back_ref[home, inside_rows, lanes]
            total = log_ref[head, span, :]
            reach = key_blocks(row_block, rows, keys, length)
            weights, pulls = [], []
            delta = jnp.zeros((rows, 1), jnp.float32)
            for block in reach:
                part = dot(queries, key_blocks_ref[block, inside_rows])
                part = jnp.exp(seen(prefix, row_block, block, rows, keys, part, MASKED) - total)
                pull = dot(attn_grad, value_blocks[block, inside_rows])
                delta = delta + jnp.sum(part * pull, axis=1, keepdims=True)
                weights.append(part)
                pulls.append(pull)
            query_grad = jnp.zeros((rows, HEAD_DIM), jnp.float32)
            for block in reach:
                key_span = pl.ds(block * keys, keys)
                score_grad = (weights[block] * (pulls[block] - delta)).astype(jnp.bfloat16)
                query_grad = query_grad + dot(score_grad, key_ref[key_span, :])
                key_grad_ref[:, key_span] += dot(queries_low, score_grad)
                value_grad_ref[:, key_span] += dot(attn_low, weights[block].astype(jnp.bfloat16))
            low, high = turn_back((query_grad * scale).T, cos_ref[:, span], sine_ref[:, span])
            query_out[home, low_rows, lanes] = low.astype(jnp.bfloat16)
            query_out[home, high_rows, lanes] = high.astype(jnp.bfloat16)
            beside(head, row_block, planned)
        for block in range(places):
            span = pl.ds(block * keys, keys)
            low, high = turn_back(key_grad_ref[:, span], cos_ref[:, span], sine_ref[:, span])
            key_out[block, low_rows] = low.astype(jnp.bfloat16)
            key_out[block, high_rows] = high.astype(jnp.bfloat16)
            value_out[block, inside_rows] = value_grad_ref[:, span].astype(jnp.bfloat16)
        begin_home(head)

    for act in left:
        act()
    for head in range(heads):
        landed_home(head)
        sent(head)
        sent_home(head)


def attend_back_heads(
    back, blocks, log_total, prefix, cos_table, sine_table, weight_grads, collective_id
):
    places, features, keys = back.shape
    heads = features // HEAD_DIM
    length = places * keys
    size = lax.axis_size("fsdp")
    shapes = [(grad.shape[0] // size, grad.shape[1]) for grad in weight_grads]
    chunks = column_chunks(shapes, 512)
    held = pl.BlockSpec(memory_space=pltpu.VMEM)
    anywhere = pl.BlockSpec(memory_space=pl.ANY)
    return pl.pallas_call(
        functools.partial(attend_back_kernel, min(256, keys), chunks, len(weight_grads)),
        out_shape=[jax.ShapeDtypeStruct(back.shape, jnp.bfloat16)] * 3
        + [jax.ShapeDtypeStruct(shape, jnp.bfloat16) for shape in shapes],
        in_specs=[pl.BlockSpec(memory_space=pltpu.SMEM)]
        + [held] * 7
        + [anywhere] * len(weight_grads),
        out_specs=[anywhere] * 3 + [held] * len(weight_grads),
        scratch_shapes=[pltpu.VMEM(back.shape, jnp.bfloat16)] * 4
        + [pltpu.VMEM((length, HEAD_DIM), jnp.bfloat16)] * 3
        + [pltpu.VMEM((HEAD_DIM, length), jnp.float32)] * 2
        + swap_scratch(heads, 1)
        + swap_scratch(heads, 3)
        + reduce_scratch(chunks, size),
        compiler_params=pltpu.CompilerParams(
            collective_id=collective_id, has_side_effects=True, vmem_limit_bytes=VMEM_LIMIT
        ),
        name="attend_back",
    )(
        prefix,
        back,
        *blocks,
        log_total,
        cos_table,
        sine_table,
        *[grad.reshape(size, shape[0], shape[1]) for grad, shape in zip(weight_grads, shapes)],
    )


def both_cores(part):
    part = part.astype(jnp.bfloat16)
    size = lax.axis_size("tp")
    other = lax.ppermute(part, "tp", [(core, (core + 1) % size) for core in range(size)])
    return part.astype(jnp.float32) + other.astype(jnp.float32)


def matmul(spec, left, right):
    return jnp.einsum(spec, left, right, preferred_element_type=jnp.float32)


def half_tables(length):
    half = HEAD_DIM // 2
    frequency = jnp.exp(jnp.arange(half, dtype=jnp.float32) * (-2.0 * math.log(BASE) / HEAD_DIM))
    angles = frequency[:, None] * jnp.arange(length, dtype=jnp.float32)[None, :]
    return jnp.cos(angles), jnp.sin(angles)


def norm_back(values, gain, grads):
    scale = lax.rsqrt(jnp.mean(values * values, axis=-1, keepdims=True) + EPS)
    pulled = grads * gain
    inner = jnp.mean(values * pulled, axis=-1, keepdims=True)
    gain_part = jnp.sum(grads * values * scale, axis=(0, 1))
    return scale * pulled - values * (scale * scale * scale * inner), gain_part


def gains_in(first, second):
    both = jnp.stack([first.reshape(4, -1), second.reshape(4, -1)], axis=1)
    both = jnp.pad(both, ((0, 0), (0, 14), (0, 128 - both.shape[2])))
    return both.reshape(64, 128).astype(jnp.bfloat16)


def gains_out(packed, which, quarter):
    return packed.reshape(-1, 16, 128)[:, which, :quarter].reshape(-1)


def heads_body(
    layer_input,
    output_cotangent,
    prefix_len,
    attn_gain,
    mlp_gain,
    query_weight,
    key_weight,
    value_weight,
    out_weight,
    gate_weight,
    up_weight,
    down_weight,
):
    block_len, seq_count, width = layer_input.shape
    places = lax.axis_size("ctx")
    ctx_index = lax.axis_index("ctx")
    local = query_weight.shape[1]
    features = seq_count * local // places
    length = places * block_len
    quarter = attn_gain.shape[0] // 4
    low = jnp.bfloat16
    shards = [
        gains_in(attn_gain, mlp_gain),
        query_weight.astype(low),
        key_weight.astype(low),
        value_weight.astype(low),
        out_weight.T.astype(low),
        gate_weight.astype(low),
        up_weight.astype(low),
        down_weight.T.astype(low),
    ]
    gains, full_query, full_key, full_value, full_out = gather_shards(shards[:5], 1)
    attn_scale = gains_out(gains, 0, quarter).astype(jnp.float32)
    mlp_scale = gains_out(gains, 1, quarter).astype(jnp.float32)
    inputs = jnp.swapaxes(layer_input, 0, 1).astype(jnp.float32)
    cotangent = jnp.swapaxes(output_cotangent, 0, 1)
    cos_table, sine_table = half_tables(length)
    own_cos = lax.dynamic_slice_in_dim(cos_table, ctx_index * block_len, block_len, 1)
    own_sine = lax.dynamic_slice_in_dim(sine_table, ctx_index * block_len, block_len, 1)
    prefix = lax.dynamic_slice_in_dim(prefix_len, ctx_index * seq_count // places, 1, 0)
    normed_low = norm_rows(inputs, attn_scale).astype(low)
    blocks_shape = (places, features, block_len)

    def project(matrix, rotated):
        product = matmul("bsd,de->bes", normed_low, matrix)
        if rotated:
            heads = product.reshape(seq_count, local // HEAD_DIM, 2, HEAD_DIM // 2, block_len)
            first, second = heads[:, :, 0], heads[:, :, 1]
            product = jnp.stack(
                [first * own_cos - second * own_sine, second * own_cos + first * own_sine], axis=2
            )
        return product.astype(low).reshape(blocks_shape)

    *blocks, mixed_low, log_total, full_gate, full_up, full_down = attend(
        project(full_query, True),
        project(full_key, True),
        project(full_value, False),
        shards[5:],
        prefix,
        2,
    )
    mixed_low = mixed_low.reshape(seq_count, local, block_len)
    hidden = inputs + both_cores(matmul("bes,de->bsd", mixed_low, full_out))
    hnorm_low = norm_rows(hidden, mlp_scale).astype(low)
    gate_out = matmul("bsd,df->bsf", hnorm_low, full_gate)
    up_out = matmul("bsd,df->bsf", hnorm_low, full_up)
    gate_sigmoid = jax.nn.sigmoid(gate_out)
    silu = gate_out * gate_sigmoid
    activated = (silu * up_out).astype(low)
    layer_output = (hidden + both_cores(matmul("bsf,df->bsd", activated, full_down))).astype(low)
    down_w_grad = matmul("bsd,bsf->df", cotangent, activated)
    act_grad = matmul("bsd,df->bsf", cotangent, full_down)
    gate_grad = (
        act_grad * up_out * (gate_sigmoid * (1.0 + gate_out * (1.0 - gate_sigmoid)))
    ).astype(low)
    up_grad = (act_grad * silu).astype(low)
    hnorm_part = matmul("bsf,df->bsd", gate_grad, full_gate) + matmul(
        "bsf,df->bsd", up_grad, full_up
    )
    hnorm_grad = both_cores(hnorm_part)
    gate_w_grad = matmul("bsd,bsf->df", hnorm_low, gate_grad)
    up_w_grad = matmul("bsd,bsf->df", hnorm_low, up_grad)
    hidden_back, mlp_gain_part = norm_back(hidden, mlp_scale, hnorm_grad)
    hidden_grad = cotangent.astype(jnp.float32) + hidden_back
    hidden_low = hidden_grad.astype(low)
    attn_grad = matmul("bsd,de->bes", hidden_low, full_out).astype(low)
    out_w_grad = matmul("bsd,bes->de", hidden_low, mixed_low)
    *grads, down, gate, up, out = attend_back_heads(
        attn_grad.reshape(blocks_shape),
        blocks,
        log_total,
        prefix,
        cos_table,
        sine_table,
        [grad.astype(low) for grad in (down_w_grad, gate_w_grad, up_w_grad, out_w_grad)],
        3,
    )
    grads = [grad.reshape(seq_count, local, block_len) for grad in grads]
    normed_part = (
        matmul("bes,de->bsd", grads[0], full_query)
        + matmul("bes,de->bsd", grads[1], full_key)
        + matmul("bes,de->bsd", grads[2], full_value)
    )
    normed_grad = both_cores(normed_part)
    input_back, attn_gain_part = norm_back(inputs, attn_scale, normed_grad)
    input_grad = (hidden_grad + input_back).astype(low)
    weight_grads = [
        matmul("bsd,bes->de", normed_low, grads[0]),
        matmul("bsd,bes->de", normed_low, grads[1]),
        matmul("bsd,bes->de", normed_low, grads[2]),
    ]
    count = lax.axis_size("fsdp")
    gain_parts = jax.vmap(gains_in)(
        attn_gain_part.reshape(count, -1), mlp_gain_part.reshape(count, -1)
    ).reshape(-1, 128)
    reduced = reduce_grads([gain_parts] + [grad.astype(low) for grad in weight_grads], 4)
    gains, query, key, value, down, gate, up, out = [
        total.astype(jnp.float32) for total in (*reduced, down, gate, up, out)
    ]
    return (
        jnp.swapaxes(layer_output, 0, 1),
        jnp.swapaxes(input_grad, 0, 1),
        gains_out(gains, 0, quarter),
        gains_out(gains, 1, quarter),
        query,
        key,
        value,
        out.T,
        gate,
        up,
        down.T,
    )


def heads_divide(mesh, args):
    block_rows = args[0].shape[0] // mesh.shape["ctx"]
    seqs = args[0].shape[1] // mesh.shape["fsdp"]
    heads = args[5].shape[1] // mesh.shape["tp"] // HEAD_DIM
    places = mesh.shape["ctx"]
    return (
        places == 4
        and mesh.shape["fsdp"] > 1
        and places % seqs == 0
        and heads % (places // seqs) == 0
        and block_rows % 256 == 0
    )


def solution(mesh):
    placed = (
        P("ctx", "fsdp", None),
        P("ctx", "fsdp", None),
        P("fsdp"),
        P("fsdp"),
        P("fsdp"),
        P("fsdp", "tp"),
        P("fsdp", "tp"),
        P("fsdp", "tp"),
        P("tp", "fsdp"),
        P("fsdp", "tp"),
        P("fsdp", "tp"),
        P("tp", "fsdp"),
    )
    def step(*args):
        chosen = heads_body if heads_divide(mesh, args) else body
        return spread_over(chosen)(*args)

    def spread_over(chosen):
      return jax.shard_map(
        chosen,
        mesh=mesh,
        in_specs=placed,
        out_specs=(
            P("ctx", "fsdp", None),
            P("ctx", "fsdp", None),
            P("fsdp"),
            P("fsdp"),
            P("fsdp", "tp"),
            P("fsdp", "tp"),
            P("fsdp", "tp"),
            P("tp", "fsdp"),
            P("fsdp", "tp"),
            P("fsdp", "tp"),
            P("tp", "fsdp"),
        ),
        check_vma=False,
    )

    return step
```
